16 devices in a mesh: rep: 4 (over y, z, core), dp: 4 (over x).
Axes of the slice: x: 4, y: 2, z: 1, core: 2. Of those that a mesh axis runs over, the one named last changes fastest.
The devices are a block of a 4x4x8 slice.
Arguments:
- x: bfloat16 [16, 4096, 640], P(('rep', 'dp')), parts along dimension 0
- dy: bfloat16 [16, 4096, 640], P(('rep', 'dp')), parts along dimension 0
- w_gate: bfloat16 [2, 640, 1536], replicated
- w_up: bfloat16 [2, 640, 1536], replicated
- w_down: bfloat16 [2, 1536, 640], replicated
- m_w_gate: float32 [2, 640, 1536], P(None, 'dp')
- m_w_up: float32 [2, 640, 1536], P(None, 'dp')
- m_w_down: float32 [2, 1536, 640], P(None, 'dp')
- v_w_gate: float32 [2, 640, 1536], P(None, 'dp')
- v_w_up: float32 [2, 640, 1536], P(None, 'dp')
- v_w_down: float32 [2, 1536, 640], P(None, 'dp')
Outputs:
- output 1: bfloat16 [8, 640, 1536], P('rep'), parts along dimension 0
- output 2: bfloat16 [8, 640, 1536], P('rep'), parts along dimension 0
- output 3: bfloat16 [8, 1536, 640], P('rep'), parts along dimension 0
- output 4: float32 [8, 640, 1536], P('rep', 'dp'), parts along dimension 0
- output 5: float32 [8, 640, 1536], P('rep', 'dp'), parts along dimension 0
- output 6: float32 [8, 1536, 640], P('rep', 'dp'), parts along dimension 0
- output 7: float32 [8, 640, 1536], P('rep', 'dp'), parts along dimension 0
- output 8: float32 [8, 640, 1536], P('rep', 'dp'), parts along dimension 0
- output 9: float32 [8, 1536, 640], P('rep', 'dp'), parts along dimension 0
There are 4 independent parts. The reference program is written for one: setup_inputs(seed, part) draws one part's arguments, and reference() takes and returns one part's arrays. A program takes and returns all parts, laid end to end along the dimension named above; an argument that names none is the same for every part.
All inputs are finite; a program needn't handle non-finite values.
Results may differ from the reference program's by a relative error of at most 0.022.
Values are sent between devices in bfloat16 or wider.
A program may use at most 768 MiB of HBM per device.

```python
import jax
import jax.numpy as jnp
from jax import lax

SEQUENCES = 4
TOKENS = 4096
D = 640
FF = 1536
LAYERS = 2
NAMES = ("w_gate", "w_up", "w_down")
SHAPES = {"w_gate": (LAYERS, D, FF), "w_up": (LAYERS, D, FF), "w_down": (LAYERS, FF, D)}


def bump(key, n, height):
    away = (jnp.arange(n, dtype=jnp.int32) - jax.random.randint(key, (), 0, n, jnp.int32)) % n
    return jnp.where(away < n // 8, height, 1.0)


def together(key, own, strength):
    shared = jax.random.normal(key, own.shape[1:], jnp.float32)
    return (own + strength * shared) * lax.rsqrt(1 + strength * strength)


def setup_inputs(seed: int = 0, part: int = 0) -> dict:
    kx, kdy, ka, kb, kz, kf, kh, kl, *keys = jax.random.split(jax.random.key(seed), 8 + 3 * len(NAMES))
    kx, kdy, ka, kb = (jax.random.fold_in(k, part) for k in (kx, kdy, ka, kb))
    kw, km, kv = (keys[i::3] for i in range(3))
    shape = (SEQUENCES, TOKENS, D)
    much_x, much_dy = jax.random.uniform(kz, (2,), jnp.float32, 0.0, 1.0)
    loud = 2.0 ** jax.random.uniform(jax.random.fold_in(kz, 1), (), jnp.float32, -1.0, 2.0)
    layers = 2.0 ** jax.random.uniform(kl, (LAYERS, 1, 1), jnp.float32, -1.0, 1.0)
    x = together(ka, jax.random.normal(kx, shape, jnp.float32), much_x) * bump(kf, D, 4.0)
    dy = together(kb, jax.random.normal(kdy, shape, jnp.float32), much_dy)
    drawn = {"x": x.astype(jnp.bfloat16), "dy": (loud * dy * (SEQUENCES * TOKENS) ** -0.5).astype(jnp.bfloat16)}
    for key, name in zip(kw, NAMES, strict=True):
        w = jax.random.normal(key, SHAPES[name], jnp.float32) * SHAPES[name][1] ** -0.5
        drawn[name] = (w * {"w_gate": 1.0, "w_up": bump(kh, FF, 4.0), "w_down": layers}[name]).astype(jnp.bfloat16)
    for key, name in zip(km, NAMES, strict=True):
        drawn[f"m_{name}"] = 0.1 * jax.random.normal(key, SHAPES[name], jnp.float32)
    for key, name in zip(kv, NAMES, strict=True):
        drawn[f"v_{name}"] = jax.random.uniform(key, SHAPES[name], jnp.float32, 0.005, 0.015)
    return drawn


def matmul(a, w):
    return jnp.dot(a, w, preferred_element_type=jnp.float32).astype(jnp.bfloat16)


def normed(h):
    wide = h.astype(jnp.float32)
    scale = lax.rsqrt(jnp.mean(wide**2, -1, keepdims=True) + 1e-6)
    return (wide * scale).astype(jnp.bfloat16)


def layer(h, w):
    a = normed(h)
    gate = jnp.dot(a, w["w_gate"], preferred_element_type=jnp.float32)
    up = jnp.dot(a, w["w_up"], preferred_element_type=jnp.float32)
    return h + matmul((jax.nn.silu(gate) * up).astype(jnp.bfloat16), w["w_down"])


def adamw(w, m, v, g):
    m = 0.9 * m + 0.1 * g
    v = 0.95 * v + 0.05 * g * g
    step = m * lax.rsqrt(v + 1e-8) + 0.1 * w
    return (w - 0.02 * step).astype(jnp.bfloat16), m, v


def clipped(gradients, sum_of_squares, count):
    factor = jnp.minimum(1.0, 0.5 * lax.rsqrt(sum_of_squares / count + 1e-30))
    return [g * factor for g in gradients]


def stack(weights, h):
    return lax.scan(lambda h, w: (layer(h, w), None), h, weights)[0]


def reference(x, dy, w_gate, w_up, w_down, m_w_gate, m_w_up, m_w_down, v_w_gate, v_w_up, v_w_down):
    weights = dict(zip(NAMES, (w_gate, w_up, w_down), strict=True))

    def take(so_far, sequence):
        h, by_y = sequence
        _, back = jax.vjp(lambda w: stack(w, h), weights)
        return jax.tree.map(lambda total, term: total + term.astype(jnp.float32), so_far, back(by_y)[0]), None

    none_yet = {name: jnp.zeros(w.shape, jnp.float32) for name, w in weights.items()}
    by_weights, _ = lax.scan(take, none_yet, (x, dy))
    gradients = [by_weights[name].astype(jnp.bfloat16).astype(jnp.float32) for name in NAMES]
    gradients = clipped(gradients, sum(jnp.sum(g * g) for g in gradients), sum(g.size for g in gradients))
    new = [
        adamw(w.astype(jnp.float32), m, v, g)
        for w, m, v, g in zip((w_gate, w_up, w_down), (m_w_gate, m_w_up, m_w_down), (v_w_gate, v_w_up, v_w_down), gradients, strict=True)
    ]
    return tuple(one[which] for which in range(3) for one in new)
```

```python
import functools

import jax
import jax.numpy as jnp
from jax import lax
from jax.experimental import pallas as pl
from jax.experimental.pallas import tpu as pltpu
from jax.sharding import PartitionSpec as P

F32, BF16 = jnp.float32, jnp.bfloat16
LANES = 128
AXIS = "dp"
MESH = pl.DeviceIdType.MESH
VMEM_LIMIT = 64000 * 1024
ROWS, COLS = (((0,), (0,)), ((), ())), (((1,), (1,)), ((), ()))


def dot(a, b):
    return jnp.dot(a, b, preferred_element_type=F32)


def dot_t(a, b):
    return lax.dot_general(a, b, COLS, preferred_element_type=F32)


def sigmoid(g):
    return 0.5 * jnp.tanh(0.5 * g) + 0.5


def normed(wide, axis):
    scale = lax.rsqrt(jnp.mean(wide * wide, axis, keepdims=True) + 1e-6)
    return (wide * scale).astype(BF16)


def forward_kernel(x_ref, dy_ref, wg_ref, wu_ref, wd_ref, a1_ref, a1t_ref, a2_ref, a2t_ref, h1t_ref, dyt_ref):
    ff = wg_ref.shape[1]
    part = 512
    dyt_ref[...] = dy_ref[...].T
    x = x_ref[...].astype(F32)
    a1 = normed(x, -1)
    a1_ref[...] = a1
    a1t_ref[...] = a1.T
    down = None
    for f in range(0, ff, part):
        gate = dot(a1, wg_ref[:, f : f + part])
        up = dot(a1, wu_ref[:, f : f + part])
        hidden = (gate * sigmoid(gate) * up).astype(BF16)
        term = dot(hidden, wd_ref[f : f + part, :])
        down = term if down is None else down + term
    h1 = (x + down.astype(BF16).astype(F32)).astype(BF16)
    h1t_ref[...] = h1.T
    a2 = normed(h1.astype(F32), -1)
    a2_ref[...] = a2
    a2t_ref[...] = a2.T


def forward(x, dy, wg, wu, wd, layer, tile=512):
    tokens, d = x.shape
    ff = wg.shape[-1]
    rows = pl.BlockSpec((tile, d), lambda t: (t, 0))
    columns = pl.BlockSpec((d, tile), lambda t: (0, t))
    weight = lambda a, b: pl.BlockSpec((None, a, b), lambda t: (layer, 0, 0))
    straight, turned = jax.ShapeDtypeStruct((tokens, d), BF16), jax.ShapeDtypeStruct((d, tokens), BF16)
    return pl.pallas_call(
        forward_kernel,
        grid=(tokens // tile,),
        in_specs=[rows, rows, weight(d, ff), weight(d, ff), weight(ff, d)],
        out_specs=[rows, columns, rows, columns, columns, columns],
        out_shape=[straight, turned, straight, turned, turned, turned],
        compiler_params=pltpu.CompilerParams(vmem_limit_bytes=VMEM_LIMIT),
        name="forward",
    )(x, dy, wg, wu, wd)


class Ring:
    def __init__(self, n, recv, summed, send_sem, recv_sem):
        self.me = lax.axis_index(AXIS)
        self.n, self.recv, self.summed, self.send_sem, self.recv_sem = n, recv, summed, send_sem, recv_sem
        self.right, self.left = (self.me + 1) % n, (self.me + n - 1) % n

    def copy(self, i, k, src, to):
        return pltpu.make_async_remote_copy(
            src_ref=src,
            dst_ref=self.recv.at[i, k],
            send_sem=self.send_sem.at[i, k],
            recv_sem=self.recv_sem.at[i, k],
            device_id={AXIS: to},
            device_id_type=MESH,
        )

    def hop(self, i, k, blocks):
        far = (self.me + 2) % self.n
        return self.copy(
            i,
            k,
            [
                lambda: blocks.at[far, 0],
                lambda: blocks.at[far, 1],
                lambda: blocks.at[self.right, 1],
                lambda: blocks.at[self.left, 0],
                lambda: self.summed.at[i, 0],
                lambda: self.summed.at[i, 1],
            ][k](),
            (self.right, self.left)[k % 2],
        )

    def start(self, i, blocks):
        for k in range(4):
            self.hop(i, k, blocks).start()

    def pass_on(self, i, blocks):
        for k, to in enumerate((self.right, self.left)):
            self.hop(i, k, blocks).wait_recv()
            self.summed[i, k] = (blocks[to, k].astype(F32) + self.recv[i, k].astype(F32)).astype(BF16)
            self.hop(i, 4 + k, blocks).start()

    def finish(self, i, blocks):
        for k in range(6):
            hop = self.hop(i, k, blocks)
            if k >= 2:
                hop.wait_recv()
            hop.wait_send()
        me = self.me
        return [
            (blocks[me, half].astype(F32) + self.recv[i, 4 + half].astype(F32) + self.recv[i, 3 - half].astype(F32)).astype(BF16)
            for half in range(2)
        ]


def pack(blocks, n, acc_g, acc_u, acc_d):
    d = acc_g.shape[0]
    half = d // n // 2
    for o in range(n):
        for h in range(2):
            rows = slice((2 * o + h) * half, (2 * o + h + 1) * half)
            blocks[o, h, 0:half, :] = acc_g[rows, :].astype(BF16)
            blocks[o, h, half : 2 * half, :] = acc_u[rows, :].astype(BF16)
            for b in range(n):
                blocks[o, h, 2 * half : 3 * half, b * LANES : (b + 1) * LANES] = acc_d[
                    (h * n + b) * half : (h * n + b + 1) * half, o * LANES : (o + 1) * LANES
                ].astype(BF16)


def unpack(halves, n, gu_ref, d_ref, ss_ref):
    half = halves[0].shape[0] // 3
    squares = jnp.zeros(ss_ref.shape, F32)
    for h, block in enumerate(halves):
        gu_ref[0, h * half : (h + 1) * half, :] = block[0:half]
        gu_ref[1, h * half : (h + 1) * half, :] = block[half : 2 * half]
        wide = block.astype(F32)
        s = jnp.sum((wide * wide).reshape(-1, 8, wide.shape[1]), axis=0)
        for b in range(n):
            squares = squares + s[:, b * LANES : (b + 1) * LANES]
            d_ref[:, (h * n + b) * half : (h * n + b + 1) * half] = block[2 * half :, b * LANES : (b + 1) * LANES].astype(F32).T.astype(BF16)
    ss_ref[...] = squares


def greet(peers):
    barrier = pltpu.get_barrier_semaphore()
    for peer in peers:
        pl.semaphore_signal(barrier, inc=1, device_id={AXIS: peer}, device_id_type=MESH)
    pl.semaphore_wait(barrier, len(peers))


def backward_kernel(n, chunks, tiles, carried, inner, *refs):
    refs = list(refs)
    take = lambda count: [refs.pop(0) for _ in range(count)]
    a_ref, at_ref, dy_ref, dyt_ref, wg_ref, wu_ref, wd_ref = take(7)
    h1t_ref = take(1)[0] if inner else None
    carried_ref = take(1)[0] if carried else None
    done = chunks - 1 + carried
    outs = [take(3) for _ in range(done)]
    last_ref = take(1)[0]
    dh_ref, dht_ref = take(2) if inner else (None, None)
    acc_g, acc_u, acc_d, blocks, recv, summed, send_sem, recv_sem = take(8)
    dat_ref = take(1)[0] if inner else None

    c, t = pl.program_id(0), pl.program_id(1)
    tile = a_ref.shape[0]
    own = wg_ref.shape[1] // n
    ring = Ring(n, recv, summed, send_sem, recv_sem)

    @pl.when((c == 0) & (t == 0))
    def _():
        greet((ring.left, ring.right))
        if carried:
            ring.start(0, carried_ref)

    places = [pl.ds(pl.multiple_of(o * own + c * LANES, LANES), LANES) for o in range(n)]
    wg = jnp.concatenate([wg_ref[:, p] for p in places], axis=1)
    wu = jnp.concatenate([wu_ref[:, p] for p in places], axis=1)
    wd = jnp.concatenate([wd_ref[p, :] for p in places], axis=0)

    a, dy = a_ref[...], dy_ref[...]
    gate, up = dot(a, wg), dot(a, wu)
    dhidden = dot_t(dy, wd).astype(BF16).astype(F32)
    s = sigmoid(gate)
    silu = gate * s
    hidden = (silu * up).astype(BF16)
    dup = (dhidden * silu).astype(BF16)
    dgate = (dhidden * up * (s + silu * (1 - s))).astype(BF16)
    at, dyt = at_ref[...], dyt_ref[...]
    accs = acc_g, acc_u, acc_d

    @pl.when(t == 0)
    def _():
        for acc in accs:
            acc[...] = jnp.zeros_like(acc)

    acc_g[...] += dot(at, dgate)
    acc_u[...] += dot(at, dup)
    acc_d[...] += dot(dyt, hidden)

    if inner:
        here = pl.ds(pl.multiple_of(t * tile, tile), tile)

        @pl.when(c == 0)
        def _():
            dat_ref[:, here] = jnp.zeros((dat_ref.shape[0], tile), F32)

        dat_ref[:, here] += dot_t(wg, dgate) + dot_t(wu, dup)

        @pl.when(c == chunks - 1)
        def _():
            da = dat_ref[:, here].astype(BF16).astype(F32)
            wide = h1t_ref[...].astype(F32)
            scale = lax.rsqrt(jnp.mean(wide * wide, 0, keepdims=True) + 1e-6)
            along = jnp.mean(da * wide, 0, keepdims=True)
            dwide = da * scale - wide * (scale * scale * scale * along)
            dht = (dyt.astype(F32) + dwide.astype(BF16).astype(F32)).astype(BF16)
            dht_ref[...] = dht
            dh_ref[...] = dht.T

    for step in range(chunks):
        i = step - 1 + carried
        if i < 0:
            continue
        source = carried_ref if carried and i == 0 else blocks.at[i - carried]

        @pl.when((c == step) & (t == tiles // 2 - 1))
        def _():
            ring.pass_on(i, source)

        @pl.when((c == step) & (t == tiles - 1))
        def _():
            unpack(ring.finish(i, source), n, *outs[i])

    for step in range(chunks - 1):

        @pl.when((c == step) & (t == tiles - 1))
        def _():
            pack(blocks.at[step], n, *accs)
            ring.start(step + carried, blocks.at[step])

    @pl.when((c == chunks - 1) & (t == tiles - 1))
    def _():
        pack(last_ref, n, *accs)


def backward(n, a, at, dy, dyt, wg, wu, wd, layer, h1t=None, carried=None, tile=1024, collective_id=0):
    tokens, d = a.shape
    ff = wg.shape[-1]
    chunks = ff // n // LANES
    tiles = tokens // tile
    inner, carry = h1t is not None, int(carried is not None)
    width, rows = n * LANES, 3 * (d // n // 2)
    done = chunks - 1 + carry
    straight = pl.BlockSpec((tile, d), lambda c, t: (t, 0))
    turned = pl.BlockSpec((d, tile), lambda c, t: (0, t))
    weight = lambda a, b: pl.BlockSpec((None, a, b), lambda c, t: (layer, 0, 0), pipeline_mode=pl.Buffered(1))
    whole = lambda *shape: pl.BlockSpec(shape, lambda c, t: (0,) * len(shape))
    once = lambda *shape: pl.BlockSpec(shape, lambda c, t: (0,) * len(shape), pipeline_mode=pl.Buffered(1))
    at_last = lambda c, t: jnp.where(c == chunks - 1, t, 0)
    packed = (n, 2, rows, width)
    in_specs = [straight, turned, straight, turned, weight(d, ff), weight(d, ff), weight(ff, d)]
    args = [a, at, dy, dyt, wg, wu, wd]
    if inner:
        in_specs.append(pl.BlockSpec((d, tile), lambda c, t: (0, at_last(c, t))))
        args.append(h1t)
    if carry:
        in_specs.append(once(*packed))
        args.append(carried)
    out_specs, out_shape = [], []
    for _ in range(done):
        for shape, dtype in (((2, d // n, width), BF16), ((LANES, d), BF16), ((8, LANES), F32)):
            out_specs.append(whole(*shape))
            out_shape.append(jax.ShapeDtypeStruct(shape, dtype))
    out_specs.append(whole(*packed))
    out_shape.append(jax.ShapeDtypeStruct(packed, BF16))
    scratch = [pltpu.VMEM((d, width), F32)] * 3 + [
        pltpu.VMEM((chunks - 1, *packed), BF16),
        pltpu.VMEM((done, 6, rows, width), BF16),
        pltpu.VMEM((done, 2, rows, width), BF16),
        pltpu.SemaphoreType.DMA((done, 6)),
        pltpu.SemaphoreType.DMA((done, 6)),
    ]
    if inner:
        out_specs += [
            pl.BlockSpec((tile, d), lambda c, t: (at_last(c, t), 0)),
            pl.BlockSpec((d, tile), lambda c, t: (0, at_last(c, t))),
        ]
        out_shape += [jax.ShapeDtypeStruct((tokens, d), BF16), jax.ShapeDtypeStruct((d, tokens), BF16)]
        scratch.append(pltpu.VMEM((d, tokens), F32))
    outs = pl.pallas_call(
        functools.partial(backward_kernel, n, chunks, tiles, carry, inner),
        grid=(chunks, tiles),
        in_specs=in_specs,
        out_specs=out_specs,
        out_shape=out_shape,
        scratch_shapes=scratch,
        compiler_params=pltpu.CompilerParams(
            vmem_limit_bytes=VMEM_LIMIT, collective_id=collective_id, has_side_effects=True,
            dimension_semantics=("arbitrary", "arbitrary"),
        ),
        name=f"backward{layer}",
    )(*args)
    sums = [tuple(outs[3 * i : 3 * i + 3]) for i in range(done)]
    return sums, outs[3 * done], outs[3 * done + 1 :]


def update_kernel(n, chunks, layers, count, *refs):
    refs = list(refs)
    take = lambda k: [refs.pop(0) for _ in range(k)]
    last_ref = take(1)[0]
    total_chunks = layers * chunks
    sums = [take(3) for _ in range(total_chunks - 1)]
    w_in, m_in, v_in = take(3), take(3), take(3)
    w_out, m_out, v_out = take(3), take(3), take(3)
    last_out = take(3)
    recv, summed, send_sem, recv_sem = take(4)
    w_own, m_own, v_own, w_new = take(3), take(3), take(3), take(3)
    ss_mine, ss_all, ss_send, ss_recv = take(4)
    load_sem, store_sem, gather_send, gather_recv = take(4)

    ring = Ring(n, recv, summed, send_sem, recv_sem)
    me = ring.me
    own_rows = [m.shape[1] for m in m_own]

    def mine(k, owner, h=None):
        rows = own_rows[k]
        if h is None:
            return pl.ds(pl.multiple_of(owner * rows, 16), rows)
        return pl.ds(pl.multiple_of(owner * rows + h * (rows // 2), 16), rows // 2)

    loads = []
    for k in range(3):
        for l in range(layers):
            i = len(loads)
            loads.append(
                (
                    pltpu.make_async_copy(w_in[k].at[l, mine(k, me)], w_own[k].at[l], load_sem.at[0, k, l]),
                    pltpu.make_async_copy(m_in[k].at[l], m_own[k].at[l], load_sem.at[1, k, l]),
                    pltpu.make_async_copy(v_in[k].at[l], v_own[k].at[l], load_sem.at[2, k, l]),
                )
            )
    for load in loads:
        for copy in load:
            copy.start()

    peers = [(me + i) % n for i in range(1, n)]
    greet(peers)
    ring.start(0, last_ref)
    ring.pass_on(0, last_ref)
    unpack(ring.finish(0, last_ref), n, *last_out)
    sums = sums[: (layers - 1) * chunks] + sums[(layers - 1) * chunks :] + [last_out]

    total = sums[0][2][...]
    for _, _, ss in sums[1:]:
        total = total + ss[...]
    ss_mine[...] = total
    shares = [
        pltpu.make_async_remote_copy(
            src_ref=ss_mine, dst_ref=ss_all.at[i], send_sem=ss_send.at[i], recv_sem=ss_recv.at[i],
            device_id={AXIS: peer}, device_id_type=MESH,
        )
        for i, peer in enumerate(peers)
    ]
    for share in shares:
        share.start()
    for share in shares:
        share.wait()
    for i in range(n - 1):
        total = total + ss_all[i]
    mean = jnp.sum(jnp.sum(total, axis=0, keepdims=True), axis=1, keepdims=True) / count
    factor = jnp.minimum(1.0, 0.5 * lax.rsqrt(mean + 1e-30))

    def gather(k, l, owner, h, way, src, to):
        return pltpu.make_async_remote_copy(
            src_ref=src,
            dst_ref=w_out[k].at[l, mine(k, owner, h)],
            send_sem=gather_send.at[k, l, h, way],
            recv_sem=gather_recv.at[k, l, h, way],
            device_id={AXIS: to},
            device_id_type=MESH,
        )

    def own_send(k, l, h, way):
        half = own_rows[k] // 2
        return gather(k, l, me, h, way, w_new[k].at[l, pl.ds(h * half, half)], (ring.right, ring.left)[way])

    def onward(k, l, way):
        owner, to = ((ring.left, ring.right), (ring.right, ring.left))[way]
        return gather(k, l, owner, way, 2, w_out[k].at[l, mine(k, owner, way)], to)

    stores = []
    order = [(k, l) for l in reversed(range(layers)) for k in range(3)]
    for k, l in order:
        for copy in loads[k * layers + l]:
            copy.wait()
        base = (layers - 1 - l) * chunks

        def step(rows, columns, g):
            g = g.astype(F32) * factor
            w, m, v = w_own[k][l, rows, columns].astype(F32), m_own[k][l, rows, columns], v_own[k][l, rows, columns]
            m = 0.9 * m + 0.1 * g
            v = 0.95 * v + 0.05 * g * g
            w_new[k][l, rows, columns] = (w - 0.02 * (m * lax.rsqrt(v + 1e-8) + 0.1 * w)).astype(BF16)
            m_own[k][l, rows, columns] = m
            v_own[k][l, rows, columns] = v

        for c in range(chunks):
            gu, gd, _ = sums[base + c]
            if k == 2:
                step(slice(c * LANES, (c + 1) * LANES), slice(None), gd[...])
            else:
                for o in range(n):
                    at = o * chunks * LANES + c * LANES
                    step(slice(None), slice(at, at + LANES), gu[k, :, o * LANES : (o + 1) * LANES])
        for h in range(2):
            for way in range(2):
                own_send(k, l, (h + way) % 2, way).start()
        for j, (src, dst) in enumerate(
            (
                (w_new[k].at[l], w_out[k].at[l, mine(k, me)]),
                (m_own[k].at[l], m_out[k].at[l]),
                (v_own[k].at[l], v_out[k].at[l]),
            )
        ):
            stores.append(pltpu.make_async_copy(src, dst, store_sem.at[j, k, l]))
            stores[-1].start()
    for k, l in order:
        for way in range(2):
            own_send(k, l, way, way).wait_recv()
            onward(k, l, way).start()
    for k, l in order:
        for way in range(2):
            own_send(k, l, 1 - way, way).wait_recv()
            onward(k, l, way).wait_recv()
            onward(k, l, way).wait_send()
            for h in range(2):
                own_send(k, l, h, way).wait_send()
    for store in stores:
        store.wait()


def update(n, last, sums, w, m, v, collective_id):
    layers = w[0].shape[0]
    chunks = w[0].shape[2] // n // LANES
    count = sum(t.size for t in w)
    packed = last.shape
    rows, width = packed[2:]
    vmem = pl.BlockSpec(memory_space=pltpu.VMEM)
    anywhere = pl.BlockSpec(memory_space=pl.ANY)
    flat = [t for one in sums for t in one]
    own = [t.shape for t in m]
    return pl.pallas_call(
        functools.partial(update_kernel, n, chunks, layers, count),
        in_specs=[vmem] * (1 + len(flat)) + [anywhere] * 9,
        out_specs=[anywhere] * 9,
        out_shape=[jax.ShapeDtypeStruct(t.shape, t.dtype) for t in (*w, *m, *v)],
        scratch_shapes=[
            pltpu.VMEM((2, w[0].shape[1] // n, width), BF16),
            pltpu.VMEM((LANES, w[0].shape[1]), BF16),
            pltpu.VMEM((8, LANES), F32),
            pltpu.VMEM((1, 6, rows, width), BF16),
            pltpu.VMEM((1, 2, rows, width), BF16),
            pltpu.SemaphoreType.DMA((1, 6)),
            pltpu.SemaphoreType.DMA((1, 6)),
            *[pltpu.VMEM(s, BF16) for s in own],
            *[pltpu.VMEM(s, F32) for s in own],
            *[pltpu.VMEM(s, F32) for s in own],
            *[pltpu.VMEM(s, BF16) for s in own],
            pltpu.VMEM((8, LANES), F32),
            pltpu.VMEM((n - 1, 8, LANES), F32),
            pltpu.SemaphoreType.DMA((n - 1,)),
            pltpu.SemaphoreType.DMA((n - 1,)),
            pltpu.SemaphoreType.DMA((3, 3, layers)),
            pltpu.SemaphoreType.DMA((3, 3, layers)),
            pltpu.SemaphoreType.DMA((3, layers, 2, 3)),
            pltpu.SemaphoreType.DMA((3, layers, 2, 3)),
        ],
        compiler_params=pltpu.CompilerParams(vmem_limit_bytes=VMEM_LIMIT, collective_id=collective_id, has_side_effects=True),
        name="update",
    )(last, *flat, *w, *m, *v)


def solution(mesh):
    n = mesh.shape[AXIS]

    def step(x, dy, *arrays):
        w, m, v = arrays[:3], arrays[3:6], arrays[6:9]
        x, dy = x.reshape(x.shape[-2:]), dy.reshape(dy.shape[-2:])
        a1, a1t, a2, a2t, h1t, dyt = forward(x, dy, *w, 0)
        sums2, last2, (dh, dht) = backward(n, a2, a2t, dy, dyt, *w, 1, h1t=h1t, collective_id=0)
        sums1, last1, _ = backward(n, a1, a1t, dh, dht, *w, 0, carried=last2, collective_id=1)
        sums = [*sums2, sums1[0], *sums1[1:]]
        return tuple(update(n, last1, sums, w, m, v, 2))

    whole, rows = P(None, None, None), P(None, AXIS, None)
    own, own_rows = P("rep", None, None), P("rep", AXIS, None)
    one = P(("rep", AXIS), None, None)
    return jax.shard_map(
        step,
        mesh=mesh,
        in_specs=(one, one, *[whole] * 3, *[rows] * 6),
        out_specs=(*[own] * 3, *[own_rows] * 6),
        check_vma=False,
    )
```

```python
import functools

import jax
import jax.numpy as jnp
from jax import lax
from jax.experimental import pallas as pl
from jax.experimental.pallas import tpu as pltpu
from jax.sharding import PartitionSpec as P

F32, BF16 = jnp.float32, jnp.bfloat16
LANES = 128
AXIS = "dp"
MESH = pl.DeviceIdType.MESH
VMEM_LIMIT = 64000 * 1024
VMEM, RESERVE = 64 * 1024 * 1024, 192 * 1024
SUB = 256
SUB_BACK = 512
TILE_INNER = 2048
ROWS, COLS = (((0,), (0,)), ((), ())), (((1,), (1,)), ((), ()))


def dot(a, b):
    return jnp.dot(a, b, preferred_element_type=F32)


def dot_t(a, b):
    return lax.dot_general(a, b, COLS, preferred_element_type=F32)


def sigmoid(g):
    return 0.5 * jnp.tanh(0.5 * g) + 0.5


def normed(wide, axis):
    scale = lax.rsqrt(jnp.mean(wide * wide, axis, keepdims=True) + 1e-6)
    return (wide * scale).astype(BF16)


def fetch(w_refs, layer, n, chunk, buffers, sems):
    copies = []
    for k, (w, buffer) in enumerate(zip(w_refs, buffers)):
        if buffer is None:
            continue
        own = w.shape[1 if k == 2 else 2] // n
        for o in range(n):
            there = pl.ds(pl.multiple_of(o * own + chunk * LANES, LANES), LANES)
            here = pl.ds(o * LANES, LANES)
            if k == 2:
                copies.append(pltpu.make_async_copy(w.at[layer, there, :], buffer.at[here, :], sems.at[k, o]))
            else:
                copies.append(pltpu.make_async_copy(w.at[layer, :, there], buffer.at[:, here], sems.at[k, o]))
    return copies


def forward_kernel(n, layer, x_ref, dy_ref, wg_ref, wu_ref, wd_ref, a1t_ref, a2_ref, a2t_ref, h1t_ref, dyt_ref, gate_ref, up_ref, wg, wu, wd, w_sem):
    chunks = wg.shape[0]
    parts = x_ref.shape[0] // SUB

    def weights(c):
        return fetch((wg_ref, wu_ref, wd_ref), layer, n, c, (wg.at[c], wu.at[c], wd.at[c]), w_sem.at[c])

    @pl.when(pl.program_id(0) == 0)
    def _():
        for c in range(chunks):
            for copy in weights(c):
                copy.start()
        for c in range(chunks):
            for copy in weights(c):
                copy.wait()

    def before(p):
        here = slice(p * SUB, (p + 1) * SUB)
        a1 = normed(x_ref[here, :].astype(F32), -1)
        a1t_ref[:, here] = a1.T
        dyt_ref[:, here] = dy_ref[here, :].T
        return a1

    def first(p, a1, c):
        here = slice(p * SUB, (p + 1) * SUB)
        gate, up = dot(a1, wg[c]), dot(a1, wu[c])
        gate_ref[c, here, :] = gate
        up_ref[c, here, :] = up
        return gate, up

    def after(p, down):
        here = slice(p * SUB, (p + 1) * SUB)
        h1 = (x_ref[here, :].astype(F32) + down.astype(BF16).astype(F32)).astype(BF16)
        h1t_ref[:, here] = h1.T
        a2 = normed(h1.astype(F32), -1)
        a2_ref[here, :] = a2
        a2t_ref[:, here] = a2.T

    todo = [(p, c) for p in range(parts) for c in range(chunks)]
    a1 = before(0)
    ahead, down = first(0, a1, 0), None
    for i, (p, c) in enumerate(todo):
        gate, up = ahead
        if i + 1 < len(todo):
            q, e = todo[i + 1]
            if q != p:
                a1 = before(q)
            ahead = first(q, a1, e)
        hidden = (gate * sigmoid(gate) * up).astype(BF16)
        term = dot(hidden, wd[c])
        down = term if c == 0 else down + term
        if c + 1 == chunks:
            after(p, down)


def forward(n, x, dy, w, layer, tile=512):
    tokens, d = x.shape
    ff = w[0].shape[-1]
    width = n * LANES
    chunks = ff // width
    rows = pl.BlockSpec((tile, d), lambda t: (t, 0))
    columns = pl.BlockSpec((d, tile), lambda t: (0, t))
    inside = pl.BlockSpec((chunks, tile, width), lambda t: (0, t, 0))
    weight = pl.BlockSpec(memory_space=pltpu.HBM)
    straight, turned = jax.ShapeDtypeStruct((tokens, d), BF16), jax.ShapeDtypeStruct((d, tokens), BF16)
    kept = jax.ShapeDtypeStruct((chunks, tokens, width), F32)
    return pl.pallas_call(
        functools.partial(forward_kernel, n, layer),
        grid=(tokens // tile,),
        in_specs=[rows, rows, weight, weight, weight],
        out_specs=[columns, rows, columns, columns, columns, inside, inside],
        out_shape=[turned, straight, turned, turned, turned, kept, kept],
        scratch_shapes=[
            pltpu.VMEM((chunks, d, width), BF16),
            pltpu.VMEM((chunks, d, width), BF16),
            pltpu.VMEM((chunks, width, d), BF16),
            pltpu.SemaphoreType.DMA((chunks, 3, n)),
        ],
        compiler_params=pltpu.CompilerParams(vmem_limit_bytes=VMEM_LIMIT),
        name="forward",
    )(x, dy, *w)


class Ring:
    def __init__(self, n, recv, summed, send_sem, recv_sem):
        self.me = lax.axis_index(AXIS)
        self.n, self.recv, self.summed, self.send_sem, self.recv_sem = n, recv, summed, send_sem, recv_sem
        self.right, self.left = (self.me + 1) % n, (self.me + n - 1) % n

    def copy(self, i, k, src, to):
        return pltpu.make_async_remote_copy(
            src_ref=src,
            dst_ref=self.recv.at[i, k],
            send_sem=self.send_sem.at[i, k],
            recv_sem=self.recv_sem.at[i, k],
            device_id={AXIS: to},
            device_id_type=MESH,
        )

    def hop(self, i, k, blocks):
        far = (self.me + 2) % self.n
        return self.copy(
            i,
            k,
            [
                lambda: blocks.at[far, 0],
                lambda: blocks.at[far, 1],
                lambda: blocks.at[self.right, 1],
                lambda: blocks.at[self.left, 0],
                lambda: self.summed.at[i, 0],
                lambda: self.summed.at[i, 1],
            ][k](),
            (self.right, self.left)[k % 2],
        )

    def start(self, i, blocks):
        for k in range(4):
            self.hop(i, k, blocks).start()

    def pass_on(self, i, blocks):
        for k, to in enumerate((self.right, self.left)):
            self.hop(i, k, blocks).wait_recv()
            self.summed[i, k] = (blocks[to, k].astype(F32) + self.recv[i, k].astype(F32)).astype(BF16)
            self.hop(i, 4 + k, blocks).start()

    def finish(self, i, blocks):
        for k in range(6):
            hop = self.hop(i, k, blocks)
            if k >= 2:
                hop.wait_recv()
            hop.wait_send()
        me = self.me
        return [
            (blocks[me, half].astype(F32) + self.recv[i, 4 + half].astype(F32) + self.recv[i, 3 - half].astype(F32)).astype(BF16)
            for half in range(2)
        ]


def pack(blocks, n, acc_g, acc_u, acc_d):
    d = acc_g.shape[0]
    half = d // n // 2
    for o in range(n):
        for h in range(2):
            rows = slice((2 * o + h) * half, (2 * o + h + 1) * half)
            blocks[o, h, 0:half, :] = acc_g[rows, :].astype(BF16)
            blocks[o, h, half : 2 * half, :] = acc_u[rows, :].astype(BF16)
            for b in range(n):
                blocks[o, h, 2 * half : 3 * half, b * LANES : (b + 1) * LANES] = acc_d[
                    (h * n + b) * half : (h * n + b + 1) * half, o * LANES : (o + 1) * LANES
                ].astype(BF16)


def unpack(halves, n, gu_ref, d_ref, ss_ref):
    half = halves[0].shape[0] // 3
    squares = jnp.zeros(ss_ref.shape, F32)
    for h, block in enumerate(halves):
        gu_ref[0, h * half : (h + 1) * half, :] = block[0:half]
        gu_ref[1, h * half : (h + 1) * half, :] = block[half : 2 * half]
        wide = block.astype(F32)
        s = jnp.sum((wide * wide).reshape(-1, 8, wide.shape[1]), axis=0)
        for b in range(n):
            squares = squares + s[:, b * LANES : (b + 1) * LANES]
            d_ref[:, (h * n + b) * half : (h * n + b + 1) * half] = block[2 * half :, b * LANES : (b + 1) * LANES].astype(F32).T.astype(BF16)
    ss_ref[...] = squares


def greet(peers):
    barrier = pltpu.get_barrier_semaphore()
    for peer in peers:
        pl.semaphore_signal(barrier, inc=1, device_id={AXIS: peer}, device_id_type=MESH)
    pl.semaphore_wait(barrier, len(peers))


def backward_kernel(n, chunks, tiles, carried, inner, layer, *refs):
    refs = list(refs)
    take = lambda count: [refs.pop(0) for _ in range(count)]
    at_ref = take(1)[0]
    if inner:
        a_ref, dy_ref, dyt_ref = take(3)
        tile = a_ref.shape[0]
    else:
        gate_ref, up_ref, dat_in, h1t_ref, outer_ref = take(5)
        tile = gate_ref.shape[0]
    w_refs = take(3)
    carried_ref = take(1)[0] if carried else None
    done = chunks - 1 + carried
    outs = [take(3) for _ in range(done)]
    last_ref = take(1)[0]
    dat_out = take(1)[0] if inner else None
    acc_g, acc_u, acc_d, blocks, recv, summed, send_sem, recv_sem = take(8)
    wd_now, w_sem = take(2)
    wg_now, wu_now = take(2) if inner else (None, None)
    if inner:
        dat_ref, dat_sem = take(2)
    else:
        dh_ref, dht_ref = take(2)

    c, t = pl.program_id(0), pl.program_id(1)
    ring = Ring(n, recv, summed, send_sem, recv_sem)

    @pl.when((c == 0) & (t == 0))
    def _():
        greet((ring.left, ring.right))
        if carried:
            ring.start(0, carried_ref)

    def weights(chunk, slot):
        buffers = [None if now is None else now.at[slot] for now in (wg_now, wu_now, wd_now)]
        return fetch(w_refs, layer, n, chunk, buffers, w_sem.at[slot])

    slot = c % 2

    @pl.when((c == 0) & (t == 0))
    def _():
        for copy in weights(0, 0):
            copy.start()

    @pl.when(t == 0)
    def _():
        for copy in weights(c, slot):
            copy.wait()

    @pl.when((t == 0) & (c < chunks - 1))
    def _():
        for copy in weights(c + 1, 1 - slot):
            copy.start()

    wd = wd_now.at[slot]
    if inner:
        wg, wu = wg_now.at[slot], wu_now.at[slot]

    accs = acc_g, acc_u, acc_d

    @pl.when(t == 0)
    def _():
        for acc in accs:
            acc[...] = jnp.zeros_like(acc)

    if inner:

        @pl.when(c == 0)
        def _():
            dat_ref[:, pl.ds(pl.multiple_of(t * tile, tile), tile)] = jnp.zeros((dat_ref.shape[0], tile), F32)

    else:

        @pl.when(c == 0)
        def _():
            for p in range(tile // LANES // 2):
                here = slice(p * 2 * LANES, (p + 1) * 2 * LANES)
                there = pl.ds(pl.multiple_of(t * tile + p * 2 * LANES, 2 * LANES), 2 * LANES)
                da = dat_in[:, here].astype(BF16).astype(F32)
                wide = h1t_ref[:, here].astype(F32)
                scale = lax.rsqrt(jnp.mean(wide * wide, 0, keepdims=True) + 1e-6)
                along = jnp.mean(da * wide, 0, keepdims=True)
                dwide = da * scale - wide * (scale * scale * scale * along)
                dht = (outer_ref[:, here].astype(F32) + dwide.astype(BF16).astype(F32)).astype(BF16)
                dht_ref[:, there] = dht
                dh_ref[there, :] = dht.T

    sub = min(tile, SUB_BACK)

    def first(p):
        rows = slice(p * sub, (p + 1) * sub)
        if not inner:
            there = pl.ds(pl.multiple_of(t * tile + p * sub, sub), sub)
            return gate_ref[rows, :], up_ref[rows, :], dot_t(dh_ref[there, :], wd[...])
        dhidden = dot_t(dy_ref[rows, :], wd[...])
        a = a_ref[rows, :]
        return dot(a, wg[...]), dot(a, wu[...]), dhidden

    def middle(gate, up, dhidden):
        dhidden = dhidden.astype(BF16).astype(F32)
        s = sigmoid(gate)
        silu = gate * s
        return (silu * up).astype(BF16), (dhidden * silu).astype(BF16), (dhidden * up * (s + silu * (1 - s))).astype(BF16)

    def second(p, hidden, dup, dgate):
        columns = slice(p * sub, (p + 1) * sub)
        here = pl.ds(pl.multiple_of(t * tile + p * sub, sub), sub)
        if inner:
            dat_ref[:, here] += dot_t(wg[...], dgate) + dot_t(wu[...], dup)
        at = at_ref[:, columns]
        acc_g[...] += dot(at, dgate)
        acc_u[...] += dot(at, dup)
        dyt = dyt_ref[:, columns] if inner else dht_ref[:, here]
        acc_d[...] += dot(dyt, hidden)

    parts = tile // sub
    ahead = first(0)
    for p in range(parts):
        now = ahead
        if p + 1 < parts:
            ahead = first(p + 1)
        second(p, *middle(*now))

    if inner:

        def keep(tile_number):
            here = pl.ds(pl.multiple_of(tile_number * tile, tile), tile)
            return pltpu.make_async_copy(dat_ref.at[:, here], dat_out.at[:, here], dat_sem.at[tile_number])

        @pl.when(c == chunks - 1)
        def _():
            keep(t).start()

        @pl.when((c == chunks - 1) & (t == tiles - 1))
        def _():
            for tile_number in range(tiles):
                keep(tile_number).wait()

    for step in range(chunks):
        i = step - 1 + carried
        if i < 0:
            continue
        source = carried_ref if carried and i == 0 else blocks.at[i - carried]
        over = (c == step) & (t == tiles - 1) if step == chunks - 1 else (c == step + 1) & (t == 0)

        @pl.when((c == step) & (t == tiles // 2 - 1))
        def _():
            ring.pass_on(i, source)

        @pl.when(over)
        def _():
            unpack(ring.finish(i, source), n, *outs[i])

    for step in range(chunks - 1):

        @pl.when((c == step) & (t == tiles - 1))
        def _():
            pack(blocks.at[step], n, *accs)
            ring.start(step + carried, blocks.at[step])

    @pl.when((c == chunks - 1) & (t == tiles - 1))
    def _():
        pack(last_ref, n, *accs)


def backward(n, at, w, layer, outer=None, kept=None, carried=None, tile=1024, collective_id=0):
    d, tokens = at.shape
    ff = w[0].shape[-1]
    width, rows = n * LANES, 3 * (d // n // 2)
    chunks = ff // width
    tiles = tokens // tile
    inner, carry = kept is None, int(carried is not None)
    done = chunks - 1 + carry
    straight = pl.BlockSpec((tile, d), lambda c, t: (t, 0))
    turned = pl.BlockSpec((d, tile), lambda c, t: (0, t))
    at_first = pl.BlockSpec((d, tile), lambda c, t: (0, jnp.where(c == 0, t, tiles - 1)))
    inside = pl.BlockSpec((None, tile, width), lambda c, t: (c, t, 0))
    hbm = pl.BlockSpec(memory_space=pltpu.HBM)
    whole = lambda *shape: pl.BlockSpec(shape, lambda c, t: (0,) * len(shape))
    once = lambda *shape: pl.BlockSpec(shape, lambda c, t: (0,) * len(shape), pipeline_mode=pl.Buffered(1))
    packed = (n, 2, rows, width)
    if inner:
        in_specs = [turned, straight, straight, turned, hbm, hbm, hbm]
        args = [at, *outer, *w]
    else:
        in_specs = [turned, inside, inside, at_first, at_first, at_first, hbm, hbm, hbm]
        args = [at, *kept, *w]
    if carry:
        in_specs.append(once(*packed))
        args.append(carried)
    out_specs, out_shape = [], []
    for _ in range(done):
        for shape, dtype in (((2, d // n, width), BF16), ((LANES, d), BF16), ((8, LANES), F32)):
            out_specs.append(whole(*shape))
            out_shape.append(jax.ShapeDtypeStruct(shape, dtype))
    out_specs.append(whole(*packed))
    out_shape.append(jax.ShapeDtypeStruct(packed, BF16))
    scratch = [pltpu.VMEM((d, width), F32)] * 3 + [
        pltpu.VMEM((chunks - 1, *packed), BF16),
        pltpu.VMEM((done, 6, rows, width), BF16),
        pltpu.VMEM((done, 2, rows, width), BF16),
        pltpu.SemaphoreType.DMA((done, 6)),
        pltpu.SemaphoreType.DMA((done, 6)),
        pltpu.VMEM((2, width, d), BF16),
        pltpu.SemaphoreType.DMA((2, 3, n)),
    ]
    if inner:
        out_specs.append(hbm)
        out_shape.append(jax.ShapeDtypeStruct((d, tokens), F32))
        scratch += [
            pltpu.VMEM((2, d, width), BF16),
            pltpu.VMEM((2, d, width), BF16),
            pltpu.VMEM((d, tokens), F32),
            pltpu.SemaphoreType.DMA((tiles,)),
        ]
    else:
        scratch += [pltpu.VMEM((tokens, d), BF16), pltpu.VMEM((d, tokens), BF16)]
    outs = pl.pallas_call(
        functools.partial(backward_kernel, n, chunks, tiles, carry, inner, layer),
        grid=(chunks, tiles),
        in_specs=in_specs,
        out_specs=out_specs,
        out_shape=out_shape,
        scratch_shapes=scratch,
        compiler_params=pltpu.CompilerParams(
            vmem_limit_bytes=VMEM_LIMIT, collective_id=collective_id, has_side_effects=True,
            dimension_semantics=("arbitrary", "arbitrary"),
        ),
        name=f"backward{layer}",
    )(*args)
    sums = [tuple(outs[3 * i : 3 * i + 3]) for i in range(done)]
    return sums, outs[3 * done], outs[3 * done + 1 :]


def update_kernel(n, chunks, layers, count, *refs):
    refs = list(refs)
    take = lambda k: [refs.pop(0) for _ in range(k)]
    last_ref = take(1)[0]
    before = layers * chunks - 1
    sums_in = [take(3) for _ in range(before)]
    w_in, m_in, v_in = take(3), take(3), take(3)
    w_out, m_own, v_own = take(3), take(3), take(3)
    last, gu_all, gd_all, squares = take(4)
    recv, summed, send_sem, recv_sem = take(4)
    w_own = take(3)
    ss_mine, ss_all, ss_send, ss_recv = take(4)
    load_sem, sums_sem, last_sem, gather_send, gather_recv = take(5)

    ring = Ring(n, recv, summed, send_sem, recv_sem)
    me = ring.me
    own_rows = [m.shape[1] for m in m_own]

    def mine(k, owner, h=None):
        rows = own_rows[k]
        if h is None:
            return pl.ds(pl.multiple_of(owner * rows, 16), rows)
        return pl.ds(pl.multiple_of(owner * rows + h * (rows // 2), 16), rows // 2)

    loads = []
    for k in range(3):
        for l in range(layers):
            i = len(loads)
            loads.append(
                (
                    pltpu.make_async_copy(w_in[k].at[l, mine(k, me)], w_own[k].at[l], load_sem.at[0, k, l]),
                    pltpu.make_async_copy(m_in[k].at[l], m_own[k].at[l], load_sem.at[1, k, l]),
                    pltpu.make_async_copy(v_in[k].at[l], v_own[k].at[l], load_sem.at[2, k, l]),
                )
            )
    for load in loads:
        for copy in load:
            copy.start()

    sum_loads = [
        pltpu.make_async_copy(src, dst.at[i], sums_sem.at[i, j])
        for i, one in enumerate(sums_in)
        for j, (src, dst) in enumerate(zip(one, (gu_all, gd_all, squares)))
    ]
    last_load = pltpu.make_async_copy(last_ref, last, last_sem)
    last_load.start()
    for copy in sum_loads:
        copy.start()

    peers = [(me + i) % n for i in range(1, n)]
    greet(peers)
    last_load.wait()
    ring.start(0, last)
    for copy in sum_loads:
        copy.wait()
    ring.pass_on(0, last)
    unpack(ring.finish(0, last), n, gu_all.at[before], gd_all.at[before], squares.at[before])

    total = squares[0]
    for i in range(before):
        total = total + squares[i + 1]
    ss_mine[...] = total
    shares = [
        pltpu.make_async_remote_copy(
            src_ref=ss_mine, dst_ref=ss_all.at[i], send_sem=ss_send.at[i], recv_sem=ss_recv.at[i],
            device_id={AXIS: peer}, device_id_type=MESH,
        )
        for i, peer in enumerate(peers)
    ]
    for share in shares:
        share.start()
    for share in shares:
        share.wait()
    for i in range(n - 1):
        total = total + ss_all[i]
    mean = jnp.sum(jnp.sum(total, axis=0, keepdims=True), axis=1, keepdims=True) / count
    factor = jnp.minimum(1.0, 0.5 * lax.rsqrt(mean + 1e-30))

    def gather(k, l, owner, h, way, src, to):
        return pltpu.make_async_remote_copy(
            src_ref=src,
            dst_ref=w_out[k].at[l, mine(k, owner, h)],
            send_sem=gather_send.at[k, l, h, way],
            recv_sem=gather_recv.at[k, l, h, way],
            device_id={AXIS: to},
            device_id_type=MESH,
        )

    def own_send(k, l, h, way):
        return gather(k, l, me, h, way, w_out[k].at[l, mine(k, me, h)], (ring.right, ring.left)[way])

    def onward(k, l, way):
        owner, to = ((ring.left, ring.right), (ring.right, ring.left))[way]
        return gather(k, l, owner, way, 2, w_out[k].at[l, mine(k, owner, way)], to)

    order = [(k, l) for l in reversed(range(layers)) for k in range(3)]
    for k, l in order:
        for copy in loads[k * layers + l]:
            copy.wait()
        base = (layers - 1 - l) * chunks

        def step(rows, columns, g):
            g = g.astype(F32) * factor
            w, m, v = w_own[k][l, rows, columns].astype(F32), m_own[k][l, rows, columns], v_own[k][l, rows, columns]
            m = 0.9 * m + 0.1 * g
            v = 0.95 * v + 0.05 * g * g
            there = pl.ds(pl.multiple_of(me * own_rows[k] + rows.start, 16), rows.stop - rows.start)
            w_out[k][l, there, columns] = (w - 0.02 * (m * lax.rsqrt(v + 1e-8) + 0.1 * w)).astype(BF16)
            m_own[k][l, rows, columns] = m
            v_own[k][l, rows, columns] = v

        for c in range(chunks):
            if k == 2:
                step(slice(c * LANES, (c + 1) * LANES), slice(None), gd_all[base + c])
            else:
                for o in range(n):
                    at = o * chunks * LANES + c * LANES
                    step(slice(0, own_rows[k]), slice(at, at + LANES), gu_all[base + c, k, :, o * LANES : (o + 1) * LANES])
        for h in range(2):
            for way in range(2):
                own_send(k, l, (h + way) % 2, way).start()
    for k, l in order:
        for way in range(2):
            own_send(k, l, way, way).wait_recv()
            onward(k, l, way).start()
    for k, l in order:
        for way in range(2):
            own_send(k, l, 1 - way, way).wait_recv()
            onward(k, l, way).wait_recv()
            onward(k, l, way).wait_send()
            for h in range(2):
                own_send(k, l, h, way).wait_send()


def update(n, last, sums, w, m, v, collective_id):
    layers = w[0].shape[0]
    chunks = w[0].shape[2] // n // LANES
    count = sum(t.size for t in w)
    packed = last.shape
    rows, width = packed[2:]
    vmem = pl.BlockSpec(memory_space=pltpu.VMEM)
    hbm = pl.BlockSpec(memory_space=pltpu.HBM)
    flat = [t for one in sums for t in one]
    own = [t.shape for t in m]
    many = layers * chunks
    return pl.pallas_call(
        functools.partial(update_kernel, n, chunks, layers, count),
        in_specs=[hbm] * (1 + len(flat) + 9),
        out_specs=[vmem] * 9,
        out_shape=[pltpu.VMEM(t.shape, t.dtype) for t in (*w, *m, *v)],
        scratch_shapes=[
            pltpu.VMEM(packed, BF16),
            pltpu.VMEM((many, 2, w[0].shape[1] // n, width), BF16),
            pltpu.VMEM((many, LANES, w[0].shape[1]), BF16),
            pltpu.VMEM((many, 8, LANES), F32),
            pltpu.VMEM((1, 6, rows, width), BF16),
            pltpu.VMEM((1, 2, rows, width), BF16),
            pltpu.SemaphoreType.DMA((1, 6)),
            pltpu.SemaphoreType.DMA((1, 6)),
            *[pltpu.VMEM(s, BF16) for s in own],
            pltpu.VMEM((8, LANES), F32),
            pltpu.VMEM((n - 1, 8, LANES), F32),
            pltpu.SemaphoreType.DMA((n - 1,)),
            pltpu.SemaphoreType.DMA((n - 1,)),
            pltpu.SemaphoreType.DMA((3, 3, layers)),
            pltpu.SemaphoreType.DMA((many - 1, 3)),
            pltpu.SemaphoreType.DMA,
            pltpu.SemaphoreType.DMA((3, layers, 2, 3)),
            pltpu.SemaphoreType.DMA((3, layers, 2, 3)),
        ],
        compiler_params=pltpu.CompilerParams(vmem_limit_bytes=VMEM - RESERVE - sum(t.size * t.dtype.itemsize for t in (*w, *m, *v)), collective_id=collective_id, has_side_effects=True),
        name="update",
    )(last, *flat, *w, *m, *v)


def put_kernel(count, *refs):
    sources, targets, sem = refs[:count], refs[count : 2 * count], refs[2 * count]
    copies = [pltpu.make_async_copy(a, b, sem.at[i]) for i, (a, b) in enumerate(zip(sources, targets))]
    for copy in copies:
        copy.start()
    for copy in copies:
        copy.wait()


def put(arrays):
    return pl.pallas_call(
        functools.partial(put_kernel, len(arrays)),
        in_specs=[pl.BlockSpec(memory_space=pltpu.VMEM)] * len(arrays),
        out_specs=[pl.BlockSpec(memory_space=pltpu.HBM)] * len(arrays),
        out_shape=[jax.ShapeDtypeStruct(t.shape, t.dtype) for t in arrays],
        scratch_shapes=[pltpu.SemaphoreType.DMA((len(arrays),))],
        compiler_params=pltpu.CompilerParams(vmem_limit_bytes=16 * 1024 * 1024),
        name="put",
    )(*arrays)


def solution(mesh):
    n = mesh.shape[AXIS]

    def step(x, dy, *arrays):
        w, m, v = arrays[:3], arrays[3:6], arrays[6:9]
        x, dy = x.reshape(x.shape[-2:]), dy.reshape(dy.shape[-2:])
        a1t, a2, a2t, h1t, dyt, *kept = forward(n, x, dy, w, 0)
        sums2, last2, (dat,) = backward(n, a2t, w, 1, outer=(a2, dy, dyt), tile=TILE_INNER, collective_id=0)
        sums1, last1, _ = backward(n, a1t, w, 0, kept=(*kept, dat, h1t, dyt), carried=last2, collective_id=1)
        sums = [*sums2, *sums1]
        return tuple(put(update(n, last1, sums, w, m, v, 2)))

    whole, rows = P(None, None, None), P(None, AXIS, None)
    own, own_rows = P("rep", None, None), P("rep", AXIS, None)
    one = P(("rep", AXIS), None, None)
    return jax.shard_map(
        step,
        mesh=mesh,
        in_specs=(one, one, *[whole] * 3, *[rows] * 6),
        out_specs=(*[own] * 3, *[own_rows] * 6),
        check_vma=False,
    )
```

```python
import functools

import jax
import jax.numpy as jnp
from jax import lax
from jax.experimental import pallas as pl
from jax.experimental.pallas import tpu as pltpu
from jax.sharding import PartitionSpec as P

F32, BF16 = jnp.float32, jnp.bfloat16
LANES = 128
AXIS = "dp"
MESH = pl.DeviceIdType.MESH
VMEM_LIMIT = 64 * 1024 * 1024 - 192 * 1024
VMEM, RESERVE = 64 * 1024 * 1024, 192 * 1024
SUB = 256
SUB_BACK = 512
ROWS, COLS = (((0,), (0,)), ((), ())), (((1,), (1,)), ((), ()))


def dot(a, b):
    return jnp.dot(a, b, preferred_element_type=F32)


def dot_t(a, b):
    return lax.dot_general(a, b, COLS, preferred_element_type=F32)


def sigmoid(g):
    return 0.5 * jnp.tanh(0.5 * g) + 0.5


def normed(wide, axis):
    scale = lax.rsqrt(jnp.mean(wide * wide, axis, keepdims=True) + 1e-6)
    return (wide * scale).astype(BF16)


def greet(peers):
    barrier = pltpu.get_barrier_semaphore()
    for peer in peers:
        pl.semaphore_signal(barrier, inc=1, device_id={AXIS: peer}, device_id_type=MESH)
    pl.semaphore_wait(barrier, len(peers))


def fetch(w_refs, layer, n, chunk, buffers, sems):
    copies = []
    for k, (w, buffer) in enumerate(zip(w_refs, buffers)):
        if buffer is None:
            continue
        own = w.shape[1 if k == 2 else 2] // n
        for o in range(n):
            there = pl.ds(pl.multiple_of(o * own + chunk * LANES, LANES), LANES)
            here = pl.ds(o * LANES, LANES)
            if k == 2:
                copies.append(pltpu.make_async_copy(w.at[layer, there, :], buffer.at[here, :], sems.at[k, o]))
            else:
                copies.append(pltpu.make_async_copy(w.at[layer, :, there], buffer.at[:, here], sems.at[k, o]))
    return copies


def forward_kernel(n, layer, early, x_ref, dy_ref, wg_ref, wu_ref, wd_ref, mg_ref, mu_ref, vg_ref, vu_ref, a1t_ref, a2_ref, a2t_ref, h1t_ref, dyt_ref, gate_ref, up_ref, near_ref, wg, wu, wd, w_sem, near_send, near_recv):
    chunks = wg.shape[0]
    parts = x_ref.shape[0] // SUB

    def weights(c):
        return fetch((wg_ref, wu_ref, wd_ref), layer, n, c, (wg.at[c], wu.at[c], wd.at[c]), w_sem.at[c])

    def moments():
        me = lax.axis_index(AXIS)
        own = mg_ref.shape[2] // n
        for side, to in enumerate(((me + 1) % n, (me + n - 1) % n)):
            for j, pair in enumerate(((mg_ref, mu_ref), (vg_ref, vu_ref))):
                for k, source in enumerate(pair):
                    for o in range(n):
                        yield pltpu.make_async_remote_copy(
                            src_ref=source.at[early, :, pl.ds(o * own, LANES)],
                            dst_ref=near_ref.at[side, j, k, :, pl.ds(o * LANES, LANES)],
                            send_sem=near_send.at[side, j, k, o],
                            recv_sem=near_recv.at[side, j, k, o],
                            device_id={AXIS: to},
                            device_id_type=MESH,
                        )

    @pl.when(pl.program_id(0) == 0)
    def _():
        for c in range(chunks):
            for copy in weights(c):
                copy.start()
        me = lax.axis_index(AXIS)
        greet(((me + n - 1) % n, (me + 1) % n))
        for copy in moments():
            copy.start()
        for c in range(chunks):
            for copy in weights(c):
                copy.wait()

    def before(p):
        here = slice(p * SUB, (p + 1) * SUB)
        a1 = normed(x_ref[here, :].astype(F32), -1)
        a1t_ref[:, here] = a1.T
        dyt_ref[:, here] = dy_ref[here, :].T
        return a1

    def first(p, a1, c):
        here = slice(p * SUB, (p + 1) * SUB)
        gate, up = dot(a1, wg[c]), dot(a1, wu[c])
        gate_ref[c, here, :] = gate
        up_ref[c, here, :] = up
        return gate, up

    def after(p, down):
        here = slice(p * SUB, (p + 1) * SUB)
        h1 = (x_ref[here, :].astype(F32) + down.astype(BF16).astype(F32)).astype(BF16)
        h1t_ref[:, here] = h1.T
        a2 = normed(h1.astype(F32), -1)
        a2_ref[here, :] = a2
        a2t_ref[:, here] = a2.T

    todo = [(p, c) for p in range(parts) for c in range(chunks)]
    a1 = before(0)
    ahead, down = first(0, a1, 0), None
    for i, (p, c) in enumerate(todo):
        gate, up = ahead
        if i + 1 < len(todo):
            q, e = todo[i + 1]
            if q != p:
                a1 = before(q)
            ahead = first(q, a1, e)
        hidden = (gate * sigmoid(gate) * up).astype(BF16)
        term = dot(hidden, wd[c])
        down = term if c == 0 else down + term
        if c + 1 == chunks:
            after(p, down)

    @pl.when(pl.program_id(0) == pl.num_programs(0) - 1)
    def _():
        for copy in moments():
            copy.wait()


def forward(n, x, dy, w, moments, layer, early, tile=512, collective_id=3):
    tokens, d = x.shape
    ff = w[0].shape[-1]
    width = n * LANES
    chunks = ff // width
    rows = pl.BlockSpec((tile, d), lambda t: (t, 0))
    columns = pl.BlockSpec((d, tile), lambda t: (0, t))
    inside = pl.BlockSpec((chunks, tile, width), lambda t: (0, t, 0))
    weight = pl.BlockSpec(memory_space=pltpu.HBM)
    straight, turned = jax.ShapeDtypeStruct((tokens, d), BF16), jax.ShapeDtypeStruct((d, tokens), BF16)
    kept = jax.ShapeDtypeStruct((chunks, tokens, width), F32)
    return pl.pallas_call(
        functools.partial(forward_kernel, n, layer, early),
        grid=(tokens // tile,),
        in_specs=[rows, rows, *[weight] * 7],
        out_specs=[columns, rows, columns, columns, columns, inside, inside, weight],
        out_shape=[turned, straight, turned, turned, turned, kept, kept, jax.ShapeDtypeStruct((2, 2, 2, d // n, width), F32)],
        scratch_shapes=[
            pltpu.VMEM((chunks, d, width), BF16),
            pltpu.VMEM((chunks, d, width), BF16),
            pltpu.VMEM((chunks, width, d), BF16),
            pltpu.SemaphoreType.DMA((chunks, 3, n)),
            pltpu.SemaphoreType.DMA((2, 2, 2, n)),
            pltpu.SemaphoreType.DMA((2, 2, 2, n)),
        ],
        compiler_params=pltpu.CompilerParams(vmem_limit_bytes=VMEM_LIMIT, collective_id=collective_id, has_side_effects=True),
        name="forward",
    )(x, dy, *w, *moments)


class Ring:
    def __init__(self, n, recv, summed, send_sem, recv_sem):
        self.me = lax.axis_index(AXIS)
        self.n, self.recv, self.summed, self.send_sem, self.recv_sem = n, recv, summed, send_sem, recv_sem
        self.right, self.left = (self.me + 1) % n, (self.me + n - 1) % n
        self.part = recv.shape[2] // 3

    def rows(self, s):
        return pl.ds(s * self.part, self.part)

    def hop(self, i, s, k, blocks):
        far, rows = (self.me + 2) % self.n, self.rows(s)
        if k >= 4:
            src = self.summed.at[i, k - 4, rows]
        else:
            src = blocks.at[(far, far, self.right, self.left)[k], (0, 1, 1, 0)[k], rows]
        return pltpu.make_async_remote_copy(
            src_ref=src,
            dst_ref=self.recv.at[i, k, rows],
            send_sem=self.send_sem.at[i, s, k],
            recv_sem=self.recv_sem.at[i, s, k],
            device_id={AXIS: (self.right, self.left)[k % 2]},
            device_id_type=MESH,
        )

    def start(self, i, blocks, parts=(0, 1, 2)):
        for k in ((0, 1), (2, 3)):
            for s in parts:
                for one in k:
                    self.hop(i, s, one, blocks).start()

    def pass_on(self, i, blocks, parts=(0, 1, 2)):
        for s in parts:
            rows = self.rows(s)
            for k, to in enumerate((self.right, self.left)):
                self.hop(i, s, k, blocks).wait_recv()
                self.summed[i, k, rows] = (blocks[to, k, rows].astype(F32) + self.recv[i, k, rows].astype(F32)).astype(BF16)
                self.hop(i, s, 4 + k, blocks).start()

    def finish(self, i, blocks):
        for s in range(3):
            for k in range(6):
                hop = self.hop(i, s, k, blocks)
                if k >= 2:
                    hop.wait_recv()
                hop.wait_send()
        me = self.me
        return [
            (blocks[me, half].astype(F32) + self.recv[i, 4 + half].astype(F32) + self.recv[i, 3 - half].astype(F32)).astype(BF16)
            for half in range(2)
        ]


def pack(blocks, n, s, acc):
    half = acc.shape[0] // n // 2
    for o in range(n):
        for h in range(2):
            if s < 2:
                blocks[o, h, s * half : (s + 1) * half, :] = acc[(2 * o + h) * half : (2 * o + h + 1) * half, :].astype(BF16)
                continue
            for b in range(n):
                blocks[o, h, s * half : (s + 1) * half, b * LANES : (b + 1) * LANES] = acc[
                    (h * n + b) * half : (h * n + b + 1) * half, o * LANES : (o + 1) * LANES
                ].astype(BF16)


def unpack(halves, n, gu_ref, d_ref, ss_ref):
    half = halves[0].shape[0] // 3
    squares = jnp.zeros(ss_ref.shape, F32)
    for h, block in enumerate(halves):
        gu_ref[0, h * half : (h + 1) * half, :] = block[0:half]
        gu_ref[1, h * half : (h + 1) * half, :] = block[half : 2 * half]
        wide = block.astype(F32)
        s = jnp.sum((wide * wide).reshape(-1, 8, wide.shape[1]), axis=0)
        for b in range(n):
            squares = squares + s[:, b * LANES : (b + 1) * LANES]
            d_ref[:, (h * n + b) * half : (h * n + b + 1) * half] = block[2 * half :, b * LANES : (b + 1) * LANES].astype(F32).T.astype(BF16)
    ss_ref[...] = squares


def through(gate, up, dhidden):
    dhidden = dhidden.astype(BF16).astype(F32)
    s = sigmoid(gate)
    silu = gate * s
    return (silu * up).astype(BF16), (dhidden * silu).astype(BF16), (dhidden * up * (s + silu * (1 - s))).astype(BF16)


def prefetch(weights, chunks, c, t):
    slot = c % 2

    @pl.when((c == 0) & (t == 0))
    def _():
        for copy in weights(0, 0):
            copy.start()

    @pl.when(t == 0)
    def _():
        for copy in weights(c, slot):
            copy.wait()

    @pl.when((t == 0) & (c < chunks - 1))
    def _():
        for copy in weights(c + 1, 1 - slot):
            copy.start()

    return slot


def inner_kernel(n, chunks, tiles, layer, *refs):
    refs = list(refs)
    take = lambda count: [refs.pop(0) for _ in range(count)]
    at_ref, a_ref, dy_ref, dyt_ref = take(4)
    w_refs = take(3)
    near_ref = take(1)[0]
    outs = take(3)
    last_ref, dat_out, far_ref, early_ref = take(4)
    acc_g, acc_u, acc_d, blocks, recv, summed, send_sem, recv_sem = take(8)
    wd_now, w_sem, wg_now, wu_now, dat_ref, dat_kept, dat_sem, mine_ref, early_send, early_recv = take(10)

    c, t = pl.program_id(0), pl.program_id(1)
    tile = a_ref.shape[0]
    ring = Ring(n, recv, summed, send_sem, recv_sem)

    def send(k, src, dst):
        return pltpu.make_async_remote_copy(
            src_ref=src,
            dst_ref=dst,
            send_sem=early_send.at[k],
            recv_sem=early_recv.at[k],
            device_id={AXIS: (ring.right, ring.left)[k % 2]},
            device_id_type=MESH,
        )

    def onward():
        return [send(k, near_ref.at[k, k], far_ref.at[k]) for k in range(2)]

    def spread():
        return [send(2 + k, mine_ref, early_ref.at[k]) for k in range(2)]

    def spread_on():
        return [send(4 + k, early_ref.at[k, k], early_ref.at[2, k]) for k in range(2)]

    @pl.when((c == 0) & (t == 0))
    def _():
        greet((ring.left, ring.right))
        for copy in onward():
            copy.start()

    @pl.when((c == 0) & (t == tiles - 1))
    def _():
        for copy in onward():
            copy.wait()

    def weights(chunk, slot):
        return fetch(w_refs, layer, n, chunk, [now.at[slot] for now in (wg_now, wu_now, wd_now)], w_sem.at[slot])

    slot = prefetch(weights, chunks, c, t)
    wg, wu, wd = wg_now.at[slot], wu_now.at[slot], wd_now.at[slot]
    accs = acc_g, acc_u, acc_d

    @pl.when(t == 0)
    def _():
        for acc in accs:
            acc[...] = jnp.zeros_like(acc)

    @pl.when(c == 0)
    def _():
        dat_ref[:, pl.ds(pl.multiple_of(t * tile, tile), tile)] = jnp.zeros((dat_ref.shape[0], tile), F32)

    def first(p):
        rows = slice(p * SUB_BACK, (p + 1) * SUB_BACK)
        a = a_ref[rows, :]
        return dot(a, wg[...]), dot(a, wu[...]), dot_t(dy_ref[rows, :], wd[...])

    def second(p, hidden, dup, dgate):
        columns = slice(p * SUB_BACK, (p + 1) * SUB_BACK)
        here = pl.ds(pl.multiple_of(t * tile + p * SUB_BACK, SUB_BACK), SUB_BACK)
        dat_ref[:, here] += dot_t(wg[...], dgate) + dot_t(wu[...], dup)
        at = at_ref[:, columns]
        acc_g[...] += dot(at, dgate)
        acc_u[...] += dot(at, dup)
        acc_d[...] += dot(dyt_ref[:, columns], hidden)

    parts = tile // SUB_BACK
    ahead = first(0)
    for p in range(parts):
        now = ahead
        if p + 1 < parts:
            ahead = first(p + 1)
        second(p, *through(*now))

    def keep(tile_number):
        here = pl.ds(pl.multiple_of(tile_number * tile, tile), tile)
        return pltpu.make_async_copy(dat_kept, dat_out.at[:, here], dat_sem.at[tile_number])

    @pl.when((c == chunks - 1) & (t > 0))
    def _():
        keep(t - 1).wait()

    @pl.when(c == chunks - 1)
    def _():
        dat_kept[...] = dat_ref[:, pl.ds(pl.multiple_of(t * tile, tile), tile)].astype(BF16)
        keep(t).start()

    @pl.when((c == chunks - 1) & (t == tiles - 1))
    def _():
        keep(t).wait()

    def end(i):
        unpack(ring.finish(i, blocks.at[i]), n, *[out.at[i] for out in outs])

    @pl.when((c > 0) & (t == 0))
    def _():
        ring.pass_on(c - 1, blocks.at[c - 1])

    @pl.when((c == 2) & (t == 0))
    def _():
        for copy in spread():
            copy.wait_recv()
        for copy in spread_on():
            copy.start()

    @pl.when((c > 0) & (t == tiles - 1))
    def _():
        end(c - 1)

    @pl.when((c == 1) & (t == tiles - 1))
    def _():
        for k in range(2):
            for h in range(2):
                mine_ref[h, k] = outs[0][0, k, h * mine_ref.shape[2] : (h + 1) * mine_ref.shape[2], :]
        for copy in spread():
            copy.start()

    @pl.when((c == chunks - 1) & (t == tiles - 1))
    def _():
        for copy in spread():
            copy.wait_send()
        for copy in spread_on():
            copy.wait()

    @pl.when((c < chunks - 1) & (t == tiles - 1))
    def _():
        for s in range(3):
            pack(blocks.at[c], n, s, accs[s])
        ring.start(c, blocks.at[c])

    @pl.when((c == chunks - 1) & (t == tiles - 1))
    def _():
        for s in range(3):
            pack(last_ref, n, s, accs[s])


def outer_kernel(n, chunks, tiles, layer, *refs):
    refs = list(refs)
    take = lambda count: [refs.pop(0) for _ in range(count)]
    at_in, gate_ref, up_ref, dat_ref, h1t_ref, dyt_ref = take(6)
    w_refs = take(3)
    carried_ref = take(1)[0]
    outs = take(3)
    acc, acc_g, blocks, recv, summed, send_sem, recv_sem = take(7)
    wd_now, w_sem, at_ref, at_sem, dh_ref, dht_ref, dup_ref, carried_sem = take(8)

    c, t = pl.program_id(0), pl.program_id(1)
    tile = gate_ref.shape[0]
    ring = Ring(n, recv, summed, send_sem, recv_sem)
    whole = pltpu.make_async_copy(at_in, at_ref, at_sem)

    @pl.when((c == 0) & (t == 0))
    def _():
        carried = pltpu.make_async_copy(carried_ref, blocks.at[0], carried_sem)
        carried.start()
        whole.start()
        greet((ring.left, ring.right))
        carried.wait()
        ring.start(0, blocks.at[0])

    def weights(chunk, slot):
        return fetch(w_refs, layer, n, chunk, [None, None, wd_now.at[slot]], w_sem.at[slot])

    wd = wd_now.at[prefetch(weights, chunks, c, t)]

    @pl.when(t == 0)
    def _():
        acc[...] = jnp.zeros_like(acc)
        acc_g[...] = jnp.zeros_like(acc_g)

    @pl.when((c == 0) & (t < tiles))
    def _():
        width = 2 * LANES
        for p in range(tile // width):
            here = slice(p * width, (p + 1) * width)
            there = pl.ds(pl.multiple_of(t * tile + p * width, width), width)
            da = dat_ref[:, here].astype(F32)
            wide = h1t_ref[:, here].astype(F32)
            scale = lax.rsqrt(jnp.mean(wide * wide, 0, keepdims=True) + 1e-6)
            along = jnp.mean(da * wide, 0, keepdims=True)
            dwide = da * scale - wide * (scale * scale * scale * along)
            dht = (dyt_ref[:, here].astype(F32) + dwide.astype(BF16).astype(F32)).astype(BF16)
            dht_ref[:, there] = dht
            dh_ref[there, :] = dht.T

    @pl.when((c == 0) & (t == 0))
    def _():
        whole.wait()

    @pl.when(t < tiles)
    def _():
        def place(p):
            return pl.ds(pl.multiple_of(t * tile + p * SUB_BACK, SUB_BACK), SUB_BACK)

        def first(p):
            rows = slice(p * SUB_BACK, (p + 1) * SUB_BACK)
            return gate_ref[rows, :], up_ref[rows, :], dot_t(dh_ref[place(p), :], wd[...])

        parts = tile // SUB_BACK
        ahead = first(0)
        for p in range(parts):
            now = ahead
            if p + 1 < parts:
                ahead = first(p + 1)
            hidden, dup, dgate = through(*now)
            dup_ref[place(p), :] = dup
            acc[...] += dot(dht_ref[:, place(p)], hidden)
            acc_g[...] += dot(at_ref[:, place(p)], dgate)

    def end(i):
        unpack(ring.finish(i, blocks.at[i]), n, *[out.at[i] for out in outs])

    @pl.when((c == 0) & (t == 1))
    def _():
        ring.pass_on(0, blocks.at[0])

    @pl.when((c > 0) & (t == 0))
    def _():
        ring.pass_on(c, blocks.at[c], (2, 0))

    @pl.when((c > 0) & (t == 2))
    def _():
        ring.pass_on(c, blocks.at[c], (1,))

    i = c + 1
    here = blocks.at[i]

    @pl.when(t == tiles - 1)
    def _():
        pack(here, n, 2, acc)
        pack(here, n, 0, acc_g)
        ring.start(i, here, (2, 0))

    @pl.when(t == tiles)
    def _():
        acc[...] = dot(at_ref[...], dup_ref[...])
        pack(here, n, 1, acc)
        ring.start(i, here, (1,))
        end(c)

    @pl.when((c == chunks - 1) & (t == tiles))
    def _():
        ring.pass_on(i, here, (2, 0, 1))
        end(i)


def sizes(n, w):
    d, ff = w[0].shape[1:]
    width, rows = n * LANES, 3 * (d // n // 2)
    return d, width, ff // width, (n, 2, rows, width)


def sums_of(count, d, n, width):
    shapes = ((count, 2, d // n, width), BF16), ((count, LANES, d), BF16), ((count, 8, LANES), F32)
    return [once(shape) for shape, _ in shapes], [jax.ShapeDtypeStruct(*one) for one in shapes]


def ring_scratch(count, packed):
    _, _, rows, width = packed
    return [
        pltpu.VMEM((count, 6, rows, width), BF16),
        pltpu.VMEM((count, 2, rows, width), BF16),
        pltpu.SemaphoreType.DMA((count, 3, 6)),
        pltpu.SemaphoreType.DMA((count, 3, 6)),
    ]


def once(shape):
    return pl.BlockSpec(shape, lambda c, t: (0,) * len(shape), pipeline_mode=pl.Buffered(1))


HBM = pl.BlockSpec(memory_space=pltpu.HBM)


def backward_inner(n, at, a, dy, dyt, w, near, layer, tile=2048, collective_id=0):
    tokens = at.shape[1]
    d, width, chunks, packed = sizes(n, w)
    tiles = tokens // tile
    straight = pl.BlockSpec((tile, d), lambda c, t: (t, 0))
    turned = pl.BlockSpec((d, tile), lambda c, t: (0, t))
    specs, shapes = sums_of(chunks - 1, d, n, width)
    early = (3, 2, 2, d // n // 2, width)
    *sums, last, dat, far, gradients = pl.pallas_call(
        functools.partial(inner_kernel, n, chunks, tiles, layer),
        grid=(chunks, tiles),
        in_specs=[turned, straight, straight, turned, HBM, HBM, HBM, HBM],
        out_specs=[*specs, once(packed), HBM, HBM, HBM],
        out_shape=[
            *shapes,
            jax.ShapeDtypeStruct(packed, BF16),
            jax.ShapeDtypeStruct((d, tokens), BF16),
            jax.ShapeDtypeStruct(near.shape[1:], F32),
            jax.ShapeDtypeStruct(early, BF16),
        ],
        scratch_shapes=[
            *[pltpu.VMEM((d, width), F32)] * 3,
            pltpu.VMEM((chunks - 1, *packed), BF16),
            *ring_scratch(chunks - 1, packed),
            pltpu.VMEM((2, width, d), BF16),
            pltpu.SemaphoreType.DMA((2, 3, n)),
            pltpu.VMEM((2, d, width), BF16),
            pltpu.VMEM((2, d, width), BF16),
            pltpu.VMEM((d, tokens), F32),
            pltpu.VMEM((d, tile), BF16),
            pltpu.SemaphoreType.DMA((tiles,)),
            pltpu.VMEM(early[1:], BF16),
            pltpu.SemaphoreType.DMA((6,)),
            pltpu.SemaphoreType.DMA((6,)),
        ],
        compiler_params=pltpu.CompilerParams(
            vmem_limit_bytes=VMEM_LIMIT, collective_id=collective_id, has_side_effects=True,
            dimension_semantics=("arbitrary", "arbitrary"),
        ),
        name="backward_inner",
    )(at, a, dy, dyt, *w, near)
    return sums, last, dat, far, gradients


def backward_outer(n, at, gate, up, dat, h1t, dyt, w, layer, carried, tile=1024, collective_id=1):
    tokens = at.shape[1]
    d, width, chunks, packed = sizes(n, w)
    tiles = tokens // tile
    at_first = pl.BlockSpec((d, tile), lambda c, t: (0, jnp.where(c == 0, jnp.minimum(t, tiles - 1), tiles - 1)))
    inside = pl.BlockSpec((None, tile, width), lambda c, t: (c, jnp.minimum(t, tiles - 1), 0))
    specs, shapes = sums_of(chunks + 1, d, n, width)
    return pl.pallas_call(
        functools.partial(outer_kernel, n, chunks, tiles, layer),
        grid=(chunks, tiles + 1),
        in_specs=[HBM, inside, inside, at_first, at_first, at_first, HBM, HBM, HBM, HBM],
        out_specs=specs,
        out_shape=shapes,
        scratch_shapes=[
            pltpu.VMEM((d, width), F32),
            pltpu.VMEM((d, width), F32),
            pltpu.VMEM((chunks + 1, *packed), BF16),
            *ring_scratch(chunks + 1, packed),
            pltpu.VMEM((2, width, d), BF16),
            pltpu.SemaphoreType.DMA((2, 3, n)),
            pltpu.VMEM((d, tokens), BF16),
            pltpu.SemaphoreType.DMA,
            pltpu.VMEM((tokens, d), BF16),
            pltpu.VMEM((d, tokens), BF16),
            pltpu.VMEM((tokens, width), BF16),
            pltpu.SemaphoreType.DMA,
        ],
        compiler_params=pltpu.CompilerParams(
            vmem_limit_bytes=VMEM_LIMIT, collective_id=collective_id, has_side_effects=True,
            dimension_semantics=("arbitrary", "arbitrary"),
        ),
        name="backward_outer",
    )(at, gate, up, dat, h1t, dyt, *w, carried)


def update_kernel(n, chunks, layers, count, *refs):
    refs = list(refs)
    take = lambda k: [refs.pop(0) for _ in range(k)]
    many = layers * chunks
    sums_in = [take(3), take(3)]
    near_in, far_in, early_in = take(3)
    w_in, m_in, v_in = take(3), take(3), take(3)
    w_out, m_own, v_own = take(3), take(3), take(3)
    gu_all, gd_all, squares = take(3)
    w_own = take(3)
    ss_mine, ss_all, ss_send, ss_recv = take(4)
    load_sem, sums_sem, gather_send, gather_recv = take(4)
    near, far, early, w_early, early_sem, w_sem = take(6)

    me = lax.axis_index(AXIS)
    right, left = (me + 1) % n, (me + n - 1) % n
    own_rows = [m.shape[1] for m in m_own]

    def mine(k, owner, h=None):
        rows = own_rows[k]
        if h is None:
            return pl.ds(pl.multiple_of(owner * rows, 16), rows)
        return pl.ds(pl.multiple_of(owner * rows + h * (rows // 2), 16), rows // 2)

    loads = []
    for k in range(3):
        for l in range(layers):
            i = len(loads)
            loads.append(
                (
                    pltpu.make_async_copy(w_in[k].at[l, mine(k, me)], w_own[k].at[l], load_sem.at[0, k, l]),
                    pltpu.make_async_copy(m_in[k].at[l], m_own[k].at[l], load_sem.at[1, k, l]),
                    pltpu.make_async_copy(v_in[k].at[l], v_own[k].at[l], load_sem.at[2, k, l]),
                )
            )
    sum_loads, done = [], 0
    for i, one in enumerate(sums_in):
        count_here = one[0].shape[0]
        for j, (src, dst) in enumerate(zip(one, (gu_all, gd_all, squares))):
            sum_loads.append(pltpu.make_async_copy(src, dst.at[pl.ds(done, count_here)], sums_sem.at[i, j]))
        done += count_here
    for copy in sum_loads:
        copy.start()
    for load in loads:
        for copy in load:
            copy.start()
    own = w_in[0].shape[2] // n
    other_loads = [
        pltpu.make_async_copy(src, dst, early_sem.at[i])
        for i, (src, dst) in enumerate(((near_in, near), (far_in, far), (early_in, early)))
    ]
    for k in range(2):
        for o in range(n):
            there = pl.ds(o * own, LANES)
            other_loads.append(
                pltpu.make_async_copy(w_in[k].at[layers - 1, :, there], w_early.at[k, :, pl.ds(o * LANES, LANES)], w_sem.at[k, o])
            )
    for copy in other_loads:
        copy.start()
    peers = [(me + i) % n for i in range(1, n)]
    greet(peers)
    for copy in sum_loads:
        copy.wait()

    total = squares[0]
    for i in range(1, many):
        total = total + squares[i]
    ss_mine[...] = total
    shares = [
        pltpu.make_async_remote_copy(
            src_ref=ss_mine, dst_ref=ss_all.at[i], send_sem=ss_send.at[i], recv_sem=ss_recv.at[i],
            device_id={AXIS: peer}, device_id_type=MESH,
        )
        for i, peer in enumerate(peers)
    ]
    for share in shares:
        share.start()
    for share in shares:
        share.wait()
    for i in range(n - 1):
        total = total + ss_all[i]
    mean = jnp.sum(jnp.sum(total, axis=0, keepdims=True), axis=1, keepdims=True) / count
    factor = jnp.minimum(1.0, 0.5 * lax.rsqrt(mean + 1e-30))

    def gather(k, l, owner, h, way, to):
        rows = mine(k, owner, h)
        if l == layers - 1 and k < 2:
            places = [(rows, pl.ds(o * own + LANES, own - LANES)) for o in range(n)]
        else:
            places = [(rows, slice(None))]
        return [
            pltpu.make_async_remote_copy(
                src_ref=w_out[k].at[l, *place],
                dst_ref=w_out[k].at[l, *place],
                send_sem=gather_send.at[k, l, h, way, i],
                recv_sem=gather_recv.at[k, l, h, way, i],
                device_id={AXIS: to},
                device_id_type=MESH,
            )
            for i, place in enumerate(places)
        ]

    def own_send(k, l, h, way):
        return gather(k, l, me, h, way, (right, left)[way])

    def onward(k, l, way):
        owner, to = ((left, right), (right, left))[way]
        return gather(k, l, owner, way, 2, to)

    def adamw(w, m, v, g):
        w, g = w.astype(F32), g.astype(F32) * factor
        m = 0.9 * m + 0.1 * g
        v = 0.95 * v + 0.05 * g * g
        return (w - 0.02 * (m * lax.rsqrt(v + 1e-8) + 0.1 * w)).astype(BF16), m, v

    order = [(k, l) for l in reversed(range(layers)) for k in range(3)]
    for k, l in order:
        for copy in loads[k * layers + l]:
            copy.wait()
        base = (layers - 1 - l) * chunks

        def step(rows, columns, g):
            there = pl.ds(pl.multiple_of(me * own_rows[k] + rows.start, 16), rows.stop - rows.start)
            w_out[k][l, there, columns], m, v = adamw(w_own[k][l, rows, columns], m_own[k][l, rows, columns], v_own[k][l, rows, columns], g)
            m_own[k][l, rows, columns] = m
            v_own[k][l, rows, columns] = v

        for c in range(chunks):
            if k == 2:
                step(slice(c * LANES, (c + 1) * LANES), slice(None), gd_all[base + c])
            else:
                for o in range(n):
                    at = o * chunks * LANES + c * LANES
                    step(slice(0, own_rows[k]), slice(at, at + LANES), gu_all[base + c, k, :, o * LANES : (o + 1) * LANES])
        for h in range(2):
            for way in range(2):
                for copy in own_send(k, l, (h + way) % 2, way):
                    copy.start()
    for copy in other_loads:
        copy.wait()
    half = own_rows[0] // 2
    for r, owner in enumerate((left, right, (me + 2) % n)):
        for k in range(2):
            for h in range(2):
                rows, there = slice(h * half, (h + 1) * half), mine(k, owner, h)
                for o in range(n):
                    columns = slice(o * LANES, (o + 1) * LANES)
                    m, v = (near[r, j, k, rows, columns] if r < 2 else far[j, k, rows, columns] for j in range(2))
                    new, _, _ = adamw(w_early[k, there, columns], m, v, early[r, h, k, :, columns])
                    w_out[k][layers - 1, there, o * own : o * own + LANES] = new
    for k, l in order:
        for way in range(2):
            for copy in own_send(k, l, way, way):
                copy.wait_recv()
            for copy in onward(k, l, way):
                copy.start()
    for k, l in order:
        for way in range(2):
            for copy in own_send(k, l, 1 - way, way):
                copy.wait_recv()
            for copy in onward(k, l, way):
                copy.wait_recv()
                copy.wait_send()
            for h in range(2):
                for copy in own_send(k, l, h, way):
                    copy.wait_send()


def update(n, sums, others, w, m, v, collective_id):
    layers = w[0].shape[0]
    chunks = w[0].shape[2] // n // LANES
    count = sum(t.size for t in w)
    width = n * LANES
    vmem = pl.BlockSpec(memory_space=pltpu.VMEM)
    own = [t.shape for t in m]
    many = layers * chunks
    return pl.pallas_call(
        functools.partial(update_kernel, n, chunks, layers, count),
        in_specs=[HBM] * (len(sums) + 12),
        out_specs=[vmem] * 9,
        out_shape=[pltpu.VMEM(t.shape, t.dtype) for t in (*w, *m, *v)],
        scratch_shapes=[
            pltpu.VMEM((many, 2, w[0].shape[1] // n, width), BF16),
            pltpu.VMEM((many, LANES, w[0].shape[1]), BF16),
            pltpu.VMEM((many, 8, LANES), F32),
            *[pltpu.VMEM(s, BF16) for s in own],
            pltpu.VMEM((8, LANES), F32),
            pltpu.VMEM((n - 1, 8, LANES), F32),
            pltpu.SemaphoreType.DMA((n - 1,)),
            pltpu.SemaphoreType.DMA((n - 1,)),
            pltpu.SemaphoreType.DMA((3, 3, layers)),
            pltpu.SemaphoreType.DMA((2, 3)),
            pltpu.SemaphoreType.DMA((3, layers, 2, 3, n)),
            pltpu.SemaphoreType.DMA((3, layers, 2, 3, n)),
            *[pltpu.VMEM(t.shape, t.dtype) for t in others],
            pltpu.VMEM((2, w[0].shape[1], width), BF16),
            pltpu.SemaphoreType.DMA((3,)),
            pltpu.SemaphoreType.DMA((2, n)),
        ],
        compiler_params=pltpu.CompilerParams(vmem_limit_bytes=VMEM - RESERVE - sum(t.size * t.dtype.itemsize for t in (*w, *m, *v)), collective_id=collective_id, has_side_effects=True),
        name="update",
    )(*sums, *others, *w, *m, *v)


def put_kernel(count, *refs):
    sources, targets, sem = refs[:count], refs[count : 2 * count], refs[2 * count]
    copies = [pltpu.make_async_copy(a, b, sem.at[i]) for i, (a, b) in enumerate(zip(sources, targets))]
    for copy in copies:
        copy.start()
    for copy in copies:
        copy.wait()


def put(arrays):
    return pl.pallas_call(
        functools.partial(put_kernel, len(arrays)),
        in_specs=[pl.BlockSpec(memory_space=pltpu.VMEM)] * len(arrays),
        out_specs=[pl.BlockSpec(memory_space=pltpu.HBM)] * len(arrays),
        out_shape=[jax.ShapeDtypeStruct(t.shape, t.dtype) for t in arrays],
        scratch_shapes=[pltpu.SemaphoreType.DMA((len(arrays),))],
        compiler_params=pltpu.CompilerParams(vmem_limit_bytes=16 * 1024 * 1024),
        name="put",
    )(*arrays)


def solution(mesh):
    n = mesh.shape[AXIS]

    def step(x, dy, *arrays):
        w, m, v = arrays[:3], arrays[3:6], arrays[6:9]
        x, dy = x.reshape(x.shape[-2:]), dy.reshape(dy.shape[-2:])
        a1t, a2, a2t, h1t, dyt, *kept, near = forward(n, x, dy, w, (*m[:2], *v[:2]), 0, 1)
        sums2, last2, dat, far, early = backward_inner(n, a2t, a2, dy, dyt, w, near, 1)
        sums1 = backward_outer(n, a1t, *kept, dat, h1t, dyt, w, 0, last2)
        return tuple(put(update(n, [*sums2, *sums1], (near, far, early), w, m, v, 2)))

    whole, rows = P(None, None, None), P(None, AXIS, None)
    own, own_rows = P("rep", None, None), P("rep", AXIS, None)
    one = P(("rep", AXIS), None, None)
    return jax.shard_map(
        step,
        mesh=mesh,
        in_specs=(one, one, *[whole] * 3, *[rows] * 6),
        out_specs=(*[own] * 3, *[own_rows] * 6),
        check_vma=False,
    )
```

```python
import functools

import jax
import jax.numpy as jnp
from jax import lax
from jax.experimental import pallas as pl
from jax.experimental.pallas import tpu as pltpu
from jax.sharding import PartitionSpec as P

F32, BF16 = jnp.float32, jnp.bfloat16
LANES = 128
AXIS = "dp"
MESH = pl.DeviceIdType.MESH
VMEM_LIMIT = 64 * 1024 * 1024 - 192 * 1024
VMEM, RESERVE = 64 * 1024 * 1024, 192 * 1024
SUB = 256
SUB_BACK = 512
ROWS, COLS = (((0,), (0,)), ((), ())), (((1,), (1,)), ((), ()))


def dot(a, b):
    return jnp.dot(a, b, preferred_element_type=F32)


def dot_t(a, b):
    return lax.dot_general(a, b, COLS, preferred_element_type=F32)


def sigmoid(g):
    return 0.5 * jnp.tanh(0.5 * g) + 0.5


def normed(wide, axis):
    scale = lax.rsqrt(jnp.mean(wide * wide, axis, keepdims=True) + 1e-6)
    return (wide * scale).astype(BF16)


def greet(peers):
    barrier = pltpu.get_barrier_semaphore()
    for peer in peers:
        pl.semaphore_signal(barrier, inc=1, device_id={AXIS: peer}, device_id_type=MESH)


def greeted(peers):
    pl.semaphore_wait(pltpu.get_barrier_semaphore(), len(peers))


def fetch(w_refs, layer, n, chunk, buffers, sems):
    copies = []
    for k, (w, buffer) in enumerate(zip(w_refs, buffers)):
        if buffer is None:
            continue
        own = w.shape[1 if k == 2 else 2] // n
        for o in range(n):
            there = pl.ds(pl.multiple_of(o * own + chunk * LANES, LANES), LANES)
            here = pl.ds(o * LANES, LANES)
            if k == 2:
                copies.append(pltpu.make_async_copy(w.at[layer, there, :], buffer.at[here, :], sems.at[k, o]))
            else:
                copies.append(pltpu.make_async_copy(w.at[layer, :, there], buffer.at[:, here], sems.at[k, o]))
    return copies


def forward_kernel(n, layer, early, x_ref, dy_ref, wg_ref, wu_ref, wd_ref, mg_ref, mu_ref, vg_ref, vu_ref, a1t_ref, a2_ref, a2t_ref, h1t_ref, dyt_ref, gate_ref, up_ref, near_ref, wg, wu, wd, w_sem, near_send, near_recv):
    chunks = wg.shape[0]
    parts = x_ref.shape[0] // SUB

    def weights(c):
        return fetch((wg_ref, wu_ref, wd_ref), layer, n, c, (wg.at[c], wu.at[c], wd.at[c]), w_sem.at[c])

    def moments():
        me = lax.axis_index(AXIS)
        own = mg_ref.shape[2] // n
        for side, to in enumerate(((me + 1) % n, (me + n - 1) % n)):
            for j, pair in enumerate(((mg_ref, mu_ref), (vg_ref, vu_ref))):
                for k, source in enumerate(pair):
                    for o in range(n):
                        yield pltpu.make_async_remote_copy(
                            src_ref=source.at[early, :, pl.ds(o * own, LANES)],
                            dst_ref=near_ref.at[side, j, k, :, pl.ds(o * LANES, LANES)],
                            send_sem=near_send.at[side, j, k, o],
                            recv_sem=near_recv.at[side, j, k, o],
                            device_id={AXIS: to},
                            device_id_type=MESH,
                        )

    @pl.when(pl.program_id(0) == 0)
    def _():
        for c in range(chunks):
            for copy in weights(c):
                copy.start()
        me = lax.axis_index(AXIS)
        greet(((me + n - 1) % n, (me + 1) % n))
        for c in range(chunks):
            for copy in weights(c):
                copy.wait()

    @pl.when(pl.program_id(0) == 1)
    def _():
        greeted((0, 1))
        for copy in moments():
            copy.start()

    def before(p):
        here = slice(p * SUB, (p + 1) * SUB)
        a1 = normed(x_ref[here, :].astype(F32), -1)
        a1t_ref[:, here] = a1.T
        dyt_ref[:, here] = dy_ref[here, :].T
        return a1

    def first(p, a1, c):
        here = slice(p * SUB, (p + 1) * SUB)
        gate, up = dot(a1, wg[c]), dot(a1, wu[c])
        gate_ref[c, here, :] = gate
        up_ref[c, here, :] = up
        return gate, up

    def after(p, down):
        here = slice(p * SUB, (p + 1) * SUB)
        h1 = (x_ref[here, :].astype(F32) + down.astype(BF16).astype(F32)).astype(BF16)
        h1t_ref[:, here] = h1.T
        a2 = normed(h1.astype(F32), -1)
        a2_ref[here, :] = a2
        a2t_ref[:, here] = a2.T

    todo = [(p, c) for p in range(parts) for c in range(chunks)]
    a1 = before(0)
    ahead, down = first(0, a1, 0), None
    for i, (p, c) in enumerate(todo):
        gate, up = ahead
        if i + 1 < len(todo):
            q, e = todo[i + 1]
            if q != p:
                a1 = before(q)
            ahead = first(q, a1, e)
        hidden = (gate * sigmoid(gate) * up).astype(BF16)
        term = dot(hidden, wd[c])
        down = term if c == 0 else down + term
        if c + 1 == chunks:
            after(p, down)

    @pl.when(pl.program_id(0) == pl.num_programs(0) - 1)
    def _():
        for copy in moments():
            copy.wait()


def forward(n, x, dy, w, moments, layer, early, tile=512, collective_id=3):
    tokens, d = x.shape
    ff = w[0].shape[-1]
    width = n * LANES
    chunks = ff // width
    rows = pl.BlockSpec((tile, d), lambda t: (t, 0))
    columns = pl.BlockSpec((d, tile), lambda t: (0, t))
    inside = pl.BlockSpec((chunks, tile, width), lambda t: (0, t, 0))
    weight = pl.BlockSpec(memory_space=pltpu.HBM)
    straight, turned = jax.ShapeDtypeStruct((tokens, d), BF16), jax.ShapeDtypeStruct((d, tokens), BF16)
    kept = jax.ShapeDtypeStruct((chunks, tokens, width), F32)
    return pl.pallas_call(
        functools.partial(forward_kernel, n, layer, early),
        grid=(tokens // tile,),
        in_specs=[rows, rows, *[weight] * 7],
        out_specs=[columns, rows, columns, columns, columns, inside, inside, weight],
        out_shape=[turned, straight, turned, turned, turned, kept, kept, jax.ShapeDtypeStruct((2, 2, 2, d // n, width), F32)],
        scratch_shapes=[
            pltpu.VMEM((chunks, d, width), BF16),
            pltpu.VMEM((chunks, d, width), BF16),
            pltpu.VMEM((chunks, width, d), BF16),
            pltpu.SemaphoreType.DMA((chunks, 3, n)),
            pltpu.SemaphoreType.DMA((2, 2, 2, n)),
            pltpu.SemaphoreType.DMA((2, 2, 2, n)),
        ],
        compiler_params=pltpu.CompilerParams(vmem_limit_bytes=VMEM_LIMIT, collective_id=collective_id, has_side_effects=True),
        name="forward",
    )(x, dy, *w, *moments)


class Ring:
    def __init__(self, n, recv, summed, send_sem, recv_sem):
        self.me = lax.axis_index(AXIS)
        self.n, self.recv, self.summed, self.send_sem, self.recv_sem = n, recv, summed, send_sem, recv_sem
        self.right, self.left = (self.me + 1) % n, (self.me + n - 1) % n
        self.part = recv.shape[2] // 3

    def rows(self, s):
        return pl.ds(s * self.part, self.part)

    def hop(self, i, s, k, blocks):
        far, rows = (self.me + 2) % self.n, self.rows(s)
        if k >= 4:
            src = self.summed.at[i, k - 4, rows]
        else:
            src = blocks.at[(far, far, self.right, self.left)[k], (0, 1, 1, 0)[k], rows]
        return pltpu.make_async_remote_copy(
            src_ref=src,
            dst_ref=self.recv.at[i, k, rows],
            send_sem=self.send_sem.at[i, s, k],
            recv_sem=self.recv_sem.at[i, s, k],
            device_id={AXIS: (self.right, self.left)[k % 2]},
            device_id_type=MESH,
        )

    def start(self, i, blocks, parts=(0, 1, 2)):
        for k in ((0, 1), (2, 3)):
            for s in parts:
                for one in k:
                    self.hop(i, s, one, blocks).start()

    def pass_on(self, i, blocks, parts=(0, 1, 2)):
        for s in parts:
            rows = self.rows(s)
            for k, to in enumerate((self.right, self.left)):
                self.hop(i, s, k, blocks).wait_recv()
                self.summed[i, k, rows] = (blocks[to, k, rows].astype(F32) + self.recv[i, k, rows].astype(F32)).astype(BF16)
                self.hop(i, s, 4 + k, blocks).start()

    def finish(self, i, blocks):
        for s in range(3):
            for k in range(6):
                hop = self.hop(i, s, k, blocks)
                if k >= 2:
                    hop.wait_recv()
                hop.wait_send()
        me = self.me
        return [
            (blocks[me, half].astype(F32) + self.recv[i, 4 + half].astype(F32) + self.recv[i, 3 - half].astype(F32)).astype(BF16)
            for half in range(2)
        ]


def pack(blocks, n, s, acc):
    half = acc.shape[0] // n // 2
    for o in range(n):
        for h in range(2):
            if s < 2:
                blocks[o, h, s * half : (s + 1) * half, :] = acc[(2 * o + h) * half : (2 * o + h + 1) * half, :].astype(BF16)
                continue
            for b in range(n):
                blocks[o, h, s * half : (s + 1) * half, b * LANES : (b + 1) * LANES] = acc[
                    (h * n + b) * half : (h * n + b + 1) * half, o * LANES : (o + 1) * LANES
                ].astype(BF16)


def unpack(halves, n, gu_ref, d_ref, ss_ref):
    half = halves[0].shape[0] // 3
    squares = jnp.zeros(ss_ref.shape, F32)
    for h, block in enumerate(halves):
        gu_ref[0, h * half : (h + 1) * half, :] = block[0:half]
        gu_ref[1, h * half : (h + 1) * half, :] = block[half : 2 * half]
        wide = block.astype(F32)
        s = jnp.sum((wide * wide).reshape(-1, 8, wide.shape[1]), axis=0)
        for b in range(n):
            squares = squares + s[:, b * LANES : (b + 1) * LANES]
            d_ref[:, (h * n + b) * half : (h * n + b + 1) * half] = block[2 * half :, b * LANES : (b + 1) * LANES].astype(F32).T.astype(BF16)
    ss_ref[...] = squares


def through(gate, up, dhidden):
    dhidden = dhidden.astype(BF16).astype(F32)
    s = sigmoid(gate)
    silu = gate * s
    return (silu * up).astype(BF16), (dhidden * silu).astype(BF16), (dhidden * up * (s + silu * (1 - s))).astype(BF16)


def prefetch(weights, chunks, c, t):
    slot = c % 2

    @pl.when((c == 0) & (t == 0))
    def _():
        for copy in weights(0, 0):
            copy.start()

    @pl.when(t == 0)
    def _():
        for copy in weights(c, slot):
            copy.wait()

    @pl.when((t == 0) & (c < chunks - 1))
    def _():
        for copy in weights(c + 1, 1 - slot):
            copy.start()

    return slot


def inner_kernel(n, chunks, tiles, layer, *refs):
    refs = list(refs)
    take = lambda count: [refs.pop(0) for _ in range(count)]
    at_ref, a_ref, dy_ref, dyt_ref = take(4)
    w_refs = take(3)
    near_ref = take(1)[0]
    outs = take(3)
    last_ref, dat_out, far_ref, early_ref = take(4)
    acc_g, acc_u, acc_d, blocks, recv, summed, send_sem, recv_sem = take(8)
    wd_now, w_sem, wg_now, wu_now, dat_ref, dat_kept, dat_sem, mine_ref, early_send, early_recv = take(10)

    c, t = pl.program_id(0), pl.program_id(1)
    tile = a_ref.shape[0]
    ring = Ring(n, recv, summed, send_sem, recv_sem)

    def send(k, src, dst):
        return pltpu.make_async_remote_copy(
            src_ref=src,
            dst_ref=dst,
            send_sem=early_send.at[k],
            recv_sem=early_recv.at[k],
            device_id={AXIS: (ring.right, ring.left)[k % 2]},
            device_id_type=MESH,
        )

    def onward():
        return [send(k, near_ref.at[k, k], far_ref.at[k]) for k in range(2)]

    def spread():
        return [send(2 + k, mine_ref, early_ref.at[k]) for k in range(2)]

    def spread_on():
        return [send(4 + k, early_ref.at[k, k], early_ref.at[2, k]) for k in range(2)]

    @pl.when((c == 0) & (t == 0))
    def _():
        greet((ring.left, ring.right))

    @pl.when((c == 0) & (t == 1))
    def _():
        greeted((ring.left, ring.right))
        for copy in onward():
            copy.start()

    def weights(chunk, slot):
        return fetch(w_refs, layer, n, chunk, [now.at[slot] for now in (wg_now, wu_now, wd_now)], w_sem.at[slot])

    slot = prefetch(weights, chunks, c, t)
    wg, wu, wd = wg_now.at[slot], wu_now.at[slot], wd_now.at[slot]
    accs = acc_g, acc_u, acc_d

    @pl.when(t == 0)
    def _():
        for acc in accs:
            acc[...] = jnp.zeros_like(acc)

    @pl.when(c == 0)
    def _():
        dat_ref[:, pl.ds(pl.multiple_of(t * tile, tile), tile)] = jnp.zeros((dat_ref.shape[0], tile), F32)

    def first(p):
        rows = slice(p * SUB_BACK, (p + 1) * SUB_BACK)
        a = a_ref[rows, :]
        return dot(a, wg[...]), dot(a, wu[...]), dot_t(dy_ref[rows, :], wd[...])

    def second(p, hidden, dup, dgate):
        columns = slice(p * SUB_BACK, (p + 1) * SUB_BACK)
        here = pl.ds(pl.multiple_of(t * tile + p * SUB_BACK, SUB_BACK), SUB_BACK)
        dat_ref[:, here] += dot_t(wg[...], dgate) + dot_t(wu[...], dup)
        at = at_ref[:, columns]
        acc_g[...] += dot(at, dgate)
        acc_u[...] += dot(at, dup)
        acc_d[...] += dot(dyt_ref[:, columns], hidden)

    parts = tile // SUB_BACK
    ahead = first(0)
    for p in range(parts):
        now = ahead
        if p + 1 < parts:
            ahead = first(p + 1)
        second(p, *through(*now))

    def keep(tile_number):
        here = pl.ds(pl.multiple_of(tile_number * tile, tile), tile)
        return pltpu.make_async_copy(dat_kept, dat_out.at[:, here], dat_sem.at[tile_number])

    @pl.when((c == chunks - 1) & (t > 0))
    def _():
        keep(t - 1).wait()

    @pl.when(c == chunks - 1)
    def _():
        dat_kept[...] = dat_ref[:, pl.ds(pl.multiple_of(t * tile, tile), tile)].astype(BF16)
        keep(t).start()

    @pl.when((c == chunks - 1) & (t == tiles - 1))
    def _():
        keep(t).wait()

    def end(i):
        unpack(ring.finish(i, blocks.at[i]), n, *[out.at[i] for out in outs])

    @pl.when((c > 0) & (t == 0))
    def _():
        ring.pass_on(c - 1, blocks.at[c - 1])

    @pl.when((c == 2) & (t == 0))
    def _():
        for copy in spread():
            copy.wait_recv()
        for copy in spread_on():
            copy.start()

    @pl.when((c > 0) & (t == tiles - 1))
    def _():
        end(c - 1)

    @pl.when((c == 1) & (t == 0))
    def _():
        for copy in onward():
            copy.wait()

    @pl.when((c == 1) & (t == tiles - 1))
    def _():
        for k in range(2):
            for h in range(2):
                mine_ref[h, k] = outs[0][0, k, h * mine_ref.shape[2] : (h + 1) * mine_ref.shape[2], :]
        for copy in spread():
            copy.start()

    @pl.when((c == chunks - 1) & (t == tiles - 1))
    def _():
        for copy in spread():
            copy.wait_send()
        for copy in spread_on():
            copy.wait()

    @pl.when((c < chunks - 1) & (t == tiles - 1))
    def _():
        for s in range(3):
            pack(blocks.at[c], n, s, accs[s])
        ring.start(c, blocks.at[c])

    @pl.when((c == chunks - 1) & (t == tiles - 1))
    def _():
        for s in range(3):
            pack(last_ref, n, s, accs[s])


def outer_kernel(n, chunks, tiles, layer, *refs):
    refs = list(refs)
    take = lambda count: [refs.pop(0) for _ in range(count)]
    at_in, gate_ref, up_ref, dat_ref, h1t_ref, dyt_ref = take(6)
    w_refs = take(3)
    carried_ref = take(1)[0]
    outs = take(3)
    acc, acc_g, blocks, recv, summed, send_sem, recv_sem = take(7)
    wd_now, w_sem, at_ref, at_sem, dh_ref, dht_ref, dup_ref, carried_sem = take(8)

    c, t = pl.program_id(0), pl.program_id(1)
    tile = gate_ref.shape[0]
    ring = Ring(n, recv, summed, send_sem, recv_sem)
    whole = pltpu.make_async_copy(at_in, at_ref, at_sem)

    @pl.when((c == 0) & (t == 0))
    def _():
        carried = pltpu.make_async_copy(carried_ref, blocks.at[0], carried_sem)
        carried.start()
        whole.start()
        greet((ring.left, ring.right))
        greeted((ring.left, ring.right))
        carried.wait()
        ring.start(0, blocks.at[0])

    def weights(chunk, slot):
        return fetch(w_refs, layer, n, chunk, [None, None, wd_now.at[slot]], w_sem.at[slot])

    wd = wd_now.at[prefetch(weights, chunks, c, t)]

    @pl.when(t == 0)
    def _():
        acc[...] = jnp.zeros_like(acc)
        acc_g[...] = jnp.zeros_like(acc_g)

    @pl.when((c == 0) & (t < tiles))
    def _():
        width = 2 * LANES
        for p in range(tile // width):
            here = slice(p * width, (p + 1) * width)
            there = pl.ds(pl.multiple_of(t * tile + p * width, width), width)
            da = dat_ref[:, here].astype(F32)
            wide = h1t_ref[:, here].astype(F32)
            scale = lax.rsqrt(jnp.mean(wide * wide, 0, keepdims=True) + 1e-6)
            along = jnp.mean(da * wide, 0, keepdims=True)
            dwide = da * scale - wide * (scale * scale * scale * along)
            dht = (dyt_ref[:, here].astype(F32) + dwide.astype(BF16).astype(F32)).astype(BF16)
            dht_ref[:, there] = dht
            dh_ref[there, :] = dht.T

    @pl.when((c == 0) & (t == 0))
    def _():
        whole.wait()

    @pl.when(t < tiles)
    def _():
        def place(p):
            return pl.ds(pl.multiple_of(t * tile + p * SUB_BACK, SUB_BACK), SUB_BACK)

        def first(p):
            rows = slice(p * SUB_BACK, (p + 1) * SUB_BACK)
            return gate_ref[rows, :], up_ref[rows, :], dot_t(dh_ref[place(p), :], wd[...])

        parts = tile // SUB_BACK
        ahead = first(0)
        for p in range(parts):
            now = ahead
            if p + 1 < parts:
                ahead = first(p + 1)
            hidden, dup, dgate = through(*now)
            dup_ref[place(p), :] = dup
            acc[...] += dot(dht_ref[:, place(p)], hidden)
            acc_g[...] += dot(at_ref[:, place(p)], dgate)

    def end(i):
        unpack(ring.finish(i, blocks.at[i]), n, *[out.at[i] for out in outs])

    @pl.when((c == 0) & (t == 1))
    def _():
        ring.pass_on(0, blocks.at[0])

    @pl.when((c > 0) & (t == 0))
    def _():
        ring.pass_on(c, blocks.at[c], (2, 0))

    @pl.when((c > 0) & (t == 2))
    def _():
        ring.pass_on(c, blocks.at[c], (1,))

    i = c + 1
    here = blocks.at[i]

    @pl.when(t == tiles - 1)
    def _():
        pack(here, n, 2, acc)
        pack(here, n, 0, acc_g)
        ring.start(i, here, (2, 0))

    @pl.when(t == tiles)
    def _():
        acc[...] = dot(at_ref[...], dup_ref[...])
        pack(here, n, 1, acc)
        ring.start(i, here, (1,))
        end(c)

    @pl.when((c == chunks - 1) & (t == tiles))
    def _():
        ring.pass_on(i, here, (2, 0, 1))
        end(i)


def sizes(n, w):
    d, ff = w[0].shape[1:]
    width, rows = n * LANES, 3 * (d // n // 2)
    return d, width, ff // width, (n, 2, rows, width)


def sums_of(count, d, n, width):
    shapes = ((count, 2, d // n, width), BF16), ((count, LANES, d), BF16), ((count, 8, LANES), F32)
    return [once(shape) for shape, _ in shapes], [jax.ShapeDtypeStruct(*one) for one in shapes]


def ring_scratch(count, packed):
    _, _, rows, width = packed
    return [
        pltpu.VMEM((count, 6, rows, width), BF16),
        pltpu.VMEM((count, 2, rows, width), BF16),
        pltpu.SemaphoreType.DMA((count, 3, 6)),
        pltpu.SemaphoreType.DMA((count, 3, 6)),
    ]


def once(shape):
    return pl.BlockSpec(shape, lambda c, t: (0,) * len(shape), pipeline_mode=pl.Buffered(1))


HBM = pl.BlockSpec(memory_space=pltpu.HBM)


def backward_inner(n, at, a, dy, dyt, w, near, layer, tile=2048, collective_id=0):
    tokens = at.shape[1]
    d, width, chunks, packed = sizes(n, w)
    tiles = tokens // tile
    straight = pl.BlockSpec((tile, d), lambda c, t: (t, 0))
    turned = pl.BlockSpec((d, tile), lambda c, t: (0, t))
    specs, shapes = sums_of(chunks - 1, d, n, width)
    early = (3, 2, 2, d // n // 2, width)
    *sums, last, dat, far, gradients = pl.pallas_call(
        functools.partial(inner_kernel, n, chunks, tiles, layer),
        grid=(chunks, tiles),
        in_specs=[turned, straight, straight, turned, HBM, HBM, HBM, HBM],
        out_specs=[*specs, once(packed), HBM, HBM, HBM],
        out_shape=[
            *shapes,
            jax.ShapeDtypeStruct(packed, BF16),
            jax.ShapeDtypeStruct((d, tokens), BF16),
            jax.ShapeDtypeStruct(near.shape[1:], F32),
            jax.ShapeDtypeStruct(early, BF16),
        ],
        scratch_shapes=[
            *[pltpu.VMEM((d, width), F32)] * 3,
            pltpu.VMEM((chunks - 1, *packed), BF16),
            *ring_scratch(chunks - 1, packed),
            pltpu.VMEM((2, width, d), BF16),
            pltpu.SemaphoreType.DMA((2, 3, n)),
            pltpu.VMEM((2, d, width), BF16),
            pltpu.VMEM((2, d, width), BF16),
            pltpu.VMEM((d, tokens), F32),
            pltpu.VMEM((d, tile), BF16),
            pltpu.SemaphoreType.DMA((tiles,)),
            pltpu.VMEM(early[1:], BF16),
            pltpu.SemaphoreType.DMA((6,)),
            pltpu.SemaphoreType.DMA((6,)),
        ],
        compiler_params=pltpu.CompilerParams(
            vmem_limit_bytes=VMEM_LIMIT, collective_id=collective_id, has_side_effects=True,
            dimension_semantics=("arbitrary", "arbitrary"),
        ),
        name="backward_inner",
    )(at, a, dy, dyt, *w, near)
    return sums, last, dat, far, gradients


def backward_outer(n, at, gate, up, dat, h1t, dyt, w, layer, carried, tile=1024, collective_id=1):
    tokens = at.shape[1]
    d, width, chunks, packed = sizes(n, w)
    tiles = tokens // tile
    at_first = pl.BlockSpec((d, tile), lambda c, t: (0, jnp.where(c == 0, jnp.minimum(t, tiles - 1), tiles - 1)))
    inside = pl.BlockSpec((None, tile, width), lambda c, t: (c, jnp.minimum(t, tiles - 1), 0))
    specs, shapes = sums_of(chunks + 1, d, n, width)
    return pl.pallas_call(
        functools.partial(outer_kernel, n, chunks, tiles, layer),
        grid=(chunks, tiles + 1),
        in_specs=[HBM, inside, inside, at_first, at_first, at_first, HBM, HBM, HBM, HBM],
        out_specs=specs,
        out_shape=shapes,
        scratch_shapes=[
            pltpu.VMEM((d, width), F32),
            pltpu.VMEM((d, width), F32),
            pltpu.VMEM((chunks + 1, *packed), BF16),
            *ring_scratch(chunks + 1, packed),
            pltpu.VMEM((2, width, d), BF16),
            pltpu.SemaphoreType.DMA((2, 3, n)),
            pltpu.VMEM((d, tokens), BF16),
            pltpu.SemaphoreType.DMA,
            pltpu.VMEM((tokens, d), BF16),
            pltpu.VMEM((d, tokens), BF16),
            pltpu.VMEM((tokens, width), BF16),
            pltpu.SemaphoreType.DMA,
        ],
        compiler_params=pltpu.CompilerParams(
            vmem_limit_bytes=VMEM_LIMIT, collective_id=collective_id, has_side_effects=True,
            dimension_semantics=("arbitrary", "arbitrary"),
        ),
        name="backward_outer",
    )(at, gate, up, dat, h1t, dyt, *w, carried)


def update_kernel(n, chunks, layers, count, *refs):
    refs = list(refs)
    take = lambda k: [refs.pop(0) for _ in range(k)]
    many = layers * chunks
    sums_in = [take(3), take(3)]
    near_in, far_in, early_in = take(3)
    w_in, m_in, v_in = take(3), take(3), take(3)
    w_out, m_own, v_own = take(3), take(3), take(3)
    gu_all, gd_all, squares = take(3)
    w_own = take(3)
    ss_mine, ss_all, ss_send, ss_recv = take(4)
    load_sem, sums_sem, gather_send, gather_recv = take(4)
    near, far, early, w_early, early_sem, w_sem = take(6)

    me = lax.axis_index(AXIS)
    right, left = (me + 1) % n, (me + n - 1) % n
    own_rows = [m.shape[1] for m in m_own]

    def mine(k, owner, h=None):
        rows = own_rows[k]
        if h is None:
            return pl.ds(pl.multiple_of(owner * rows, 16), rows)
        return pl.ds(pl.multiple_of(owner * rows + h * (rows // 2), 16), rows // 2)

    loads = []
    for k in range(3):
        for l in range(layers):
            i = len(loads)
            loads.append(
                (
                    pltpu.make_async_copy(w_in[k].at[l, mine(k, me)], w_own[k].at[l], load_sem.at[0, k, l]),
                    pltpu.make_async_copy(m_in[k].at[l], m_own[k].at[l], load_sem.at[1, k, l]),
                    pltpu.make_async_copy(v_in[k].at[l], v_own[k].at[l], load_sem.at[2, k, l]),
                )
            )
    sum_loads, done = [], 0
    for i, one in enumerate(sums_in):
        count_here = one[0].shape[0]
        for j, (src, dst) in enumerate(zip(one, (gu_all, gd_all, squares))):
            sum_loads.append(pltpu.make_async_copy(src, dst.at[pl.ds(done, count_here)], sums_sem.at[i, j]))
        done += count_here
    for copy in sum_loads:
        copy.start()
    at_once = layers - 1
    for copy in loads[at_once]:
        copy.start()
    own = w_in[0].shape[2] // n
    other_loads = [
        pltpu.make_async_copy(src, dst, early_sem.at[i])
        for i, (src, dst) in enumerate(((near_in, near), (far_in, far), (early_in, early)))
    ]
    for k in range(2):
        for o in range(n):
            there = pl.ds(o * own, LANES)
            other_loads.append(
                pltpu.make_async_copy(w_in[k].at[layers - 1, :, there], w_early.at[k, :, pl.ds(o * LANES, LANES)], w_sem.at[k, o])
            )
    peers = [(me + i) % n for i in range(1, n)]
    greet(peers)
    greeted(peers)
    for copy in sum_loads:
        copy.wait()

    total = squares[0]
    for i in range(1, many):
        total = total + squares[i]
    ss_mine[...] = total
    shares = [
        pltpu.make_async_remote_copy(
            src_ref=ss_mine, dst_ref=ss_all.at[i], send_sem=ss_send.at[i], recv_sem=ss_recv.at[i],
            device_id={AXIS: peer}, device_id_type=MESH,
        )
        for i, peer in enumerate(peers)
    ]
    for share in shares:
        share.start()
    for i, load in enumerate(loads):
        if i != at_once:
            for copy in load:
                copy.start()
    for copy in other_loads:
        copy.start()
    for share in shares:
        share.wait()
    for i in range(n - 1):
        total = total + ss_all[i]
    mean = jnp.sum(jnp.sum(total, axis=0, keepdims=True), axis=1, keepdims=True) / count
    factor = jnp.minimum(1.0, 0.5 * lax.rsqrt(mean + 1e-30))

    def gather(k, l, owner, h, way, to):
        rows = mine(k, owner, h)
        if l == layers - 1 and k < 2:
            places = [(rows, pl.ds(o * own + LANES, own - LANES)) for o in range(n)]
        else:
            places = [(rows, slice(None))]
        return [
            pltpu.make_async_remote_copy(
                src_ref=w_out[k].at[l, *place],
                dst_ref=w_out[k].at[l, *place],
                send_sem=gather_send.at[k, l, h, way, i],
                recv_sem=gather_recv.at[k, l, h, way, i],
                device_id={AXIS: to},
                device_id_type=MESH,
            )
            for i, place in enumerate(places)
        ]

    def own_send(k, l, h, way):
        return gather(k, l, me, h, way, (right, left)[way])

    def onward(k, l, way):
        owner, to = ((left, right), (right, left))[way]
        return gather(k, l, owner, way, 2, to)

    def adamw(w, m, v, g):
        w, g = w.astype(F32), g.astype(F32) * factor
        m = 0.9 * m + 0.1 * g
        v = 0.95 * v + 0.05 * g * g
        return (w - 0.02 * (m * lax.rsqrt(v + 1e-8) + 0.1 * w)).astype(BF16), m, v

    order = [(k, l) for l in reversed(range(layers)) for k in range(3)]
    for k, l in order:
        for copy in loads[k * layers + l]:
            copy.wait()
        base = (layers - 1 - l) * chunks

        def step(rows, columns, g):
            there = pl.ds(pl.multiple_of(me * own_rows[k] + rows.start, 16), rows.stop - rows.start)
            w_out[k][l, there, columns], m, v = adamw(w_own[k][l, rows, columns], m_own[k][l, rows, columns], v_own[k][l, rows, columns], g)
            m_own[k][l, rows, columns] = m
            v_own[k][l, rows, columns] = v

        for c in range(chunks):
            if k == 2:
                step(slice(c * LANES, (c + 1) * LANES), slice(None), gd_all[base + c])
            else:
                for o in range(n):
                    at = o * chunks * LANES + c * LANES
                    step(slice(0, own_rows[k]), slice(at, at + LANES), gu_all[base + c, k, :, o * LANES : (o + 1) * LANES])
        for h in range(2):
            for way in range(2):
                for copy in own_send(k, l, (h + way) % 2, way):
                    copy.start()
    for copy in other_loads:
        copy.wait()
    half = own_rows[0] // 2
    for r, owner in enumerate((left, right, (me + 2) % n)):
        for k in range(2):
            for h in range(2):
                rows, there = slice(h * half, (h + 1) * half), mine(k, owner, h)
                for o in range(n):
                    columns = slice(o * LANES, (o + 1) * LANES)
                    m, v = (near[r, j, k, rows, columns] if r < 2 else far[j, k, rows, columns] for j in range(2))
                    new, _, _ = adamw(w_early[k, there, columns], m, v, early[r, h, k, :, columns])
                    w_out[k][layers - 1, there, o * own : o * own + LANES] = new
    for k, l in order:
        for way in range(2):
            for copy in own_send(k, l, way, way):
                copy.wait_recv()
            for copy in onward(k, l, way):
                copy.start()
    for k, l in order:
        for way in range(2):
            for copy in own_send(k, l, 1 - way, way):
                copy.wait_recv()
            for copy in onward(k, l, way):
                copy.wait_recv()
                copy.wait_send()
            for h in range(2):
                for copy in own_send(k, l, h, way):
                    copy.wait_send()


def update(n, sums, others, w, m, v, collective_id):
    layers = w[0].shape[0]
    chunks = w[0].shape[2] // n // LANES
    count = sum(t.size for t in w)
    width = n * LANES
    vmem = pl.BlockSpec(memory_space=pltpu.VMEM)
    own = [t.shape for t in m]
    many = layers * chunks
    return pl.pallas_call(
        functools.partial(update_kernel, n, chunks, layers, count),
        in_specs=[HBM] * (len(sums) + 12),
        out_specs=[vmem] * 9,
        out_shape=[pltpu.VMEM(t.shape, t.dtype) for t in (*w, *m, *v)],
        scratch_shapes=[
            pltpu.VMEM((many, 2, w[0].shape[1] // n, width), BF16),
            pltpu.VMEM((many, LANES, w[0].shape[1]), BF16),
            pltpu.VMEM((many, 8, LANES), F32),
            *[pltpu.VMEM(s, BF16) for s in own],
            pltpu.VMEM((8, LANES), F32),
            pltpu.VMEM((n - 1, 8, LANES), F32),
            pltpu.SemaphoreType.DMA((n - 1,)),
            pltpu.SemaphoreType.DMA((n - 1,)),
            pltpu.SemaphoreType.DMA((3, 3, layers)),
            pltpu.SemaphoreType.DMA((2, 3)),
            pltpu.SemaphoreType.DMA((3, layers, 2, 3, n)),
            pltpu.SemaphoreType.DMA((3, layers, 2, 3, n)),
            *[pltpu.VMEM(t.shape, t.dtype) for t in others],
            pltpu.VMEM((2, w[0].shape[1], width), BF16),
            pltpu.SemaphoreType.DMA((3,)),
            pltpu.SemaphoreType.DMA((2, n)),
        ],
        compiler_params=pltpu.CompilerParams(vmem_limit_bytes=VMEM - RESERVE - sum(t.size * t.dtype.itemsize for t in (*w, *m, *v)), collective_id=collective_id, has_side_effects=True),
        name="update",
    )(*sums, *others, *w, *m, *v)


def put_kernel(count, *refs):
    sources, targets, sem = refs[:count], refs[count : 2 * count], refs[2 * count]
    copies = [pltpu.make_async_copy(a, b, sem.at[i]) for i, (a, b) in enumerate(zip(sources, targets))]
    for copy in copies:
        copy.start()
    for copy in copies:
        copy.wait()


def put(arrays):
    return pl.pallas_call(
        functools.partial(put_kernel, len(arrays)),
        in_specs=[pl.BlockSpec(memory_space=pltpu.VMEM)] * len(arrays),
        out_specs=[pl.BlockSpec(memory_space=pltpu.HBM)] * len(arrays),
        out_shape=[jax.ShapeDtypeStruct(t.shape, t.dtype) for t in arrays],
        scratch_shapes=[pltpu.SemaphoreType.DMA((len(arrays),))],
        compiler_params=pltpu.CompilerParams(vmem_limit_bytes=16 * 1024 * 1024),
        name="put",
    )(*arrays)


def solution(mesh):
    n = mesh.shape[AXIS]

    def step(x, dy, *arrays):
        w, m, v = arrays[:3], arrays[3:6], arrays[6:9]
        x, dy = x.reshape(x.shape[-2:]), dy.reshape(dy.shape[-2:])
        a1t, a2, a2t, h1t, dyt, *kept, near = forward(n, x, dy, w, (*m[:2], *v[:2]), 0, 1)
        sums2, last2, dat, far, early = backward_inner(n, a2t, a2, dy, dyt, w, near, 1)
        sums1 = backward_outer(n, a1t, *kept, dat, h1t, dyt, w, 0, last2)
        return tuple(put(update(n, [*sums2, *sums1], (near, far, early), w, m, v, 2)))

    whole, rows = P(None, None, None), P(None, AXIS, None)
    own, own_rows = P("rep", None, None), P("rep", AXIS, None)
    one = P(("rep", AXIS), None, None)
    return jax.shard_map(
        step,
        mesh=mesh,
        in_specs=(one, one, *[whole] * 3, *[rows] * 6),
        out_specs=(*[own] * 3, *[own_rows] * 6),
        check_vma=False,
    )
```

```python
import functools

import jax
import jax.numpy as jnp
from jax import lax
from jax.experimental import pallas as pl
from jax.experimental.pallas import tpu as pltpu
from jax.sharding import PartitionSpec as P

F32, BF16 = jnp.float32, jnp.bfloat16
LANES = 128
AXIS = "dp"
MESH = pl.DeviceIdType.MESH
VMEM_LIMIT = 64 * 1024 * 1024 - 192 * 1024
VMEM, RESERVE = 64 * 1024 * 1024, 192 * 1024
SUB = 256
SUB_BACK = 512
ROWS, COLS = (((0,), (0,)), ((), ())), (((1,), (1,)), ((), ()))


def dot(a, b):
    return jnp.dot(a, b, preferred_element_type=F32)


def dot_t(a, b):
    return lax.dot_general(a, b, COLS, preferred_element_type=F32)


def sigmoid(g):
    return 0.5 * jnp.tanh(0.5 * g) + 0.5


def normed(wide, axis):
    scale = lax.rsqrt(jnp.mean(wide * wide, axis, keepdims=True) + 1e-6)
    return (wide * scale).astype(BF16)


def greet(peers):
    barrier = pltpu.get_barrier_semaphore()
    for peer in peers:
        pl.semaphore_signal(barrier, inc=1, device_id={AXIS: peer}, device_id_type=MESH)


def greeted(peers):
    pl.semaphore_wait(pltpu.get_barrier_semaphore(), len(peers))


def fetch(w_refs, layer, n, chunk, buffers, sems):
    copies = []
    for k, (w, buffer) in enumerate(zip(w_refs, buffers)):
        if buffer is None:
            continue
        own = w.shape[1 if k == 2 else 2] // n
        for o in range(n):
            there = pl.ds(pl.multiple_of(o * own + chunk * LANES, LANES), LANES)
            here = pl.ds(o * LANES, LANES)
            if k == 2:
                copies.append(pltpu.make_async_copy(w.at[layer, there, :], buffer.at[here, :], sems.at[k, o]))
            else:
                copies.append(pltpu.make_async_copy(w.at[layer, :, there], buffer.at[:, here], sems.at[k, o]))
    return copies


def forward_kernel(n, layer, early, x_ref, dy_ref, wg_ref, wu_ref, wd_ref, mg_ref, mu_ref, vg_ref, vu_ref, a1t_ref, a2_ref, a2t_ref, h1t_ref, dyt_ref, gate_ref, up_ref, near_ref, wg, wu, wd, w_sem, near_send, near_recv):
    chunks = wg.shape[0]
    parts = x_ref.shape[0] // SUB

    def weights(c):
        return fetch((wg_ref, wu_ref, wd_ref), layer, n, c, (wg.at[c], wu.at[c], wd.at[c]), w_sem.at[c])

    def moments():
        me = lax.axis_index(AXIS)
        own = mg_ref.shape[2] // n
        for side, to in enumerate(((me + 1) % n, (me + n - 1) % n)):
            for j, pair in enumerate(((mg_ref, mu_ref), (vg_ref, vu_ref))):
                for k, source in enumerate(pair):
                    for o in range(n):
                        yield pltpu.make_async_remote_copy(
                            src_ref=source.at[early, :, pl.ds(o * own, LANES)],
                            dst_ref=near_ref.at[side, j, k, :, pl.ds(o * LANES, LANES)],
                            send_sem=near_send.at[side, j, k, o],
                            recv_sem=near_recv.at[side, j, k, o],
                            device_id={AXIS: to},
                            device_id_type=MESH,
                        )

    @pl.when(pl.program_id(0) == 0)
    def _():
        for c in range(chunks):
            for copy in weights(c):
                copy.start()
        me = lax.axis_index(AXIS)
        greet(((me + n - 1) % n, (me + 1) % n))
        for c in range(chunks):
            for copy in weights(c):
                copy.wait()

    @pl.when(pl.program_id(0) == 1)
    def _():
        greeted((0, 1))
        for copy in moments():
            copy.start()

    def before(p):
        here = slice(p * SUB, (p + 1) * SUB)
        a1 = normed(x_ref[here, :].astype(F32), -1)
        a1t_ref[:, here] = a1.T
        dyt_ref[:, here] = dy_ref[here, :].T
        return a1

    def first(p, a1, c):
        here = slice(p * SUB, (p + 1) * SUB)
        gate, up = dot(a1, wg[c]), dot(a1, wu[c])
        gate_ref[c, here, :] = gate
        up_ref[c, here, :] = up
        return gate, up

    def after(p, down):
        here = slice(p * SUB, (p + 1) * SUB)
        h1 = (x_ref[here, :].astype(F32) + down.astype(BF16).astype(F32)).astype(BF16)
        h1t_ref[:, here] = h1.T
        a2 = normed(h1.astype(F32), -1)
        a2_ref[here, :] = a2
        a2t_ref[:, here] = a2.T

    todo = [(p, c) for p in range(parts) for c in range(chunks)]
    a1 = before(0)
    ahead, down = first(0, a1, 0), None
    for i, (p, c) in enumerate(todo):
        gate, up = ahead
        if i + 1 < len(todo):
            q, e = todo[i + 1]
            if q != p:
                a1 = before(q)
            ahead = first(q, a1, e)
        hidden = (gate * sigmoid(gate) * up).astype(BF16)
        term = dot(hidden, wd[c])
        down = term if c == 0 else down + term
        if c + 1 == chunks:
            after(p, down)

    @pl.when(pl.program_id(0) == pl.num_programs(0) - 1)
    def _():
        for copy in moments():
            copy.wait()


def forward(n, x, dy, w, moments, layer, early, tile=512, collective_id=3):
    tokens, d = x.shape
    ff = w[0].shape[-1]
    width = n * LANES
    chunks = ff // width
    rows = pl.BlockSpec((tile, d), lambda t: (t, 0))
    columns = pl.BlockSpec((d, tile), lambda t: (0, t))
    inside = pl.BlockSpec((chunks, tile, width), lambda t: (0, t, 0))
    weight = pl.BlockSpec(memory_space=pltpu.HBM)
    straight, turned = jax.ShapeDtypeStruct((tokens, d), BF16), jax.ShapeDtypeStruct((d, tokens), BF16)
    kept = jax.ShapeDtypeStruct((chunks, tokens, width), F32)
    return pl.pallas_call(
        functools.partial(forward_kernel, n, layer, early),
        grid=(tokens // tile,),
        in_specs=[rows, rows, *[weight] * 7],
        out_specs=[columns, rows, columns, columns, columns, inside, inside, weight],
        out_shape=[turned, straight, turned, turned, turned, kept, kept, jax.ShapeDtypeStruct((2, 2, 2, d // n, width), F32)],
        scratch_shapes=[
            pltpu.VMEM((chunks, d, width), BF16),
            pltpu.VMEM((chunks, d, width), BF16),
            pltpu.VMEM((chunks, width, d), BF16),
            pltpu.SemaphoreType.DMA((chunks, 3, n)),
            pltpu.SemaphoreType.DMA((2, 2, 2, n)),
            pltpu.SemaphoreType.DMA((2, 2, 2, n)),
        ],
        compiler_params=pltpu.CompilerParams(vmem_limit_bytes=VMEM_LIMIT, collective_id=collective_id, has_side_effects=True),
        name="forward",
    )(x, dy, *w, *moments)


class Ring:
    def __init__(self, n, recv, summed, send_sem, recv_sem):
        self.me = lax.axis_index(AXIS)
        self.n, self.recv, self.summed, self.send_sem, self.recv_sem = n, recv, summed, send_sem, recv_sem
        self.right, self.left = (self.me + 1) % n, (self.me + n - 1) % n
        self.part = recv.shape[2] // 3

    def rows(self, s):
        return pl.ds(s * self.part, self.part)

    def hop(self, i, s, k, blocks):
        far, rows = (self.me + 2) % self.n, self.rows(s)
        if k >= 4:
            src = self.summed.at[i, k - 4, rows]
        else:
            src = blocks.at[(far, far, self.right, self.left)[k], (0, 1, 1, 0)[k], rows]
        return pltpu.make_async_remote_copy(
            src_ref=src,
            dst_ref=self.recv.at[i, k, rows],
            send_sem=self.send_sem.at[i, s, k],
            recv_sem=self.recv_sem.at[i, s, k],
            device_id={AXIS: (self.right, self.left)[k % 2]},
            device_id_type=MESH,
        )

    def start(self, i, blocks, parts=(0, 1, 2)):
        for k in ((0, 1), (2, 3)):
            for s in parts:
                for one in k:
                    self.hop(i, s, one, blocks).start()

    def pass_on(self, i, blocks, parts=(0, 1, 2)):
        for s in parts:
            rows = self.rows(s)
            for k, to in enumerate((self.right, self.left)):
                self.hop(i, s, k, blocks).wait_recv()
                self.summed[i, k, rows] = (blocks[to, k, rows].astype(F32) + self.recv[i, k, rows].astype(F32)).astype(BF16)
                self.hop(i, s, 4 + k, blocks).start()

    def finish(self, i, blocks):
        for s in range(3):
            for k in range(6):
                hop = self.hop(i, s, k, blocks)
                if k >= 2:
                    hop.wait_recv()
                hop.wait_send()
        me = self.me
        return [
            (blocks[me, half].astype(F32) + self.recv[i, 4 + half].astype(F32) + self.recv[i, 3 - half].astype(F32)).astype(BF16)
            for half in range(2)
        ]


def pack(blocks, n, s, acc):
    half = acc.shape[0] // n // 2
    for o in range(n):
        for h in range(2):
            if s < 2:
                blocks[o, h, s * half : (s + 1) * half, :] = acc[(2 * o + h) * half : (2 * o + h + 1) * half, :].astype(BF16)
                continue
            for b in range(n):
                blocks[o, h, s * half : (s + 1) * half, b * LANES : (b + 1) * LANES] = acc[
                    (h * n + b) * half : (h * n + b + 1) * half, o * LANES : (o + 1) * LANES
                ].astype(BF16)


def unpack(halves, n, gu_ref, d_ref, ss_ref):
    half = halves[0].shape[0] // 3
    squares = jnp.zeros(ss_ref.shape, F32)
    for h, block in enumerate(halves):
        gu_ref[0, h * half : (h + 1) * half, :] = block[0:half]
        gu_ref[1, h * half : (h + 1) * half, :] = block[half : 2 * half]
        wide = block.astype(F32)
        s = jnp.sum((wide * wide).reshape(-1, 8, wide.shape[1]), axis=0)
        for b in range(n):
            squares = squares + s[:, b * LANES : (b + 1) * LANES]
            d_ref[:, (h * n + b) * half : (h * n + b + 1) * half] = block[2 * half :, b * LANES : (b + 1) * LANES].astype(F32).T.astype(BF16)
    ss_ref[...] = squares


def through(gate, up, dhidden):
    dhidden = dhidden.astype(BF16).astype(F32)
    s = sigmoid(gate)
    silu = gate * s
    return (silu * up).astype(BF16), (dhidden * silu).astype(BF16), (dhidden * up * (s + silu * (1 - s))).astype(BF16)


def prefetch(weights, chunks, c, t):
    slot = c % 2

    @pl.when((c == 0) & (t == 0))
    def _():
        for copy in weights(0, 0):
            copy.start()

    @pl.when(t == 0)
    def _():
        for copy in weights(c, slot):
            copy.wait()

    @pl.when((t == 0) & (c < chunks - 1))
    def _():
        for copy in weights(c + 1, 1 - slot):
            copy.start()

    return slot


def inner_kernel(n, chunks, tiles, layer, *refs):
    refs = list(refs)
    take = lambda count: [refs.pop(0) for _ in range(count)]
    at_ref, a_ref, dy_ref, dyt_ref = take(4)
    w_refs = take(3)
    near_ref = take(1)[0]
    outs = take(3)
    last_ref, dat_out, far_ref, early_ref = take(4)
    acc_g, acc_u, acc_d, blocks, recv, summed, send_sem, recv_sem = take(8)
    wd_now, w_sem, wg_now, wu_now, dat_ref, dat_kept, dat_sem, mine_ref, early_send, early_recv = take(10)

    c, t = pl.program_id(0), pl.program_id(1)
    tile = a_ref.shape[0]
    ring = Ring(n, recv, summed, send_sem, recv_sem)

    def send(k, src, dst):
        return pltpu.make_async_remote_copy(
            src_ref=src,
            dst_ref=dst,
            send_sem=early_send.at[k],
            recv_sem=early_recv.at[k],
            device_id={AXIS: (ring.right, ring.left)[k % 2]},
            device_id_type=MESH,
        )

    def onward():
        return [send(k, near_ref.at[k, k], far_ref.at[k]) for k in range(2)]

    def spread():
        return [send(2 + k, mine_ref, early_ref.at[k]) for k in range(2)]

    def spread_on():
        return [send(4 + k, early_ref.at[k, k], early_ref.at[2, k]) for k in range(2)]

    @pl.when((c == 0) & (t == 0))
    def _():
        greet((ring.left, ring.right))

    @pl.when((c == 0) & (t == 1))
    def _():
        greeted((ring.left, ring.right))
        for copy in onward():
            copy.start()

    def weights(chunk, slot):
        return fetch(w_refs, layer, n, chunk, [now.at[slot] for now in (wg_now, wu_now, wd_now)], w_sem.at[slot])

    slot = prefetch(weights, chunks, c, t)
    wg, wu, wd = wg_now.at[slot], wu_now.at[slot], wd_now.at[slot]
    accs = acc_g, acc_u, acc_d

    @pl.when(t == 0)
    def _():
        for acc in accs:
            acc[...] = jnp.zeros_like(acc)

    @pl.when(c == 0)
    def _():
        dat_ref[:, pl.ds(pl.multiple_of(t * tile, tile), tile)] = jnp.zeros((dat_ref.shape[0], tile), F32)

    def first(p):
        rows = slice(p * SUB_BACK, (p + 1) * SUB_BACK)
        a = a_ref[rows, :]
        return dot(a, wg[...]), dot(a, wu[...]), dot_t(dy_ref[rows, :], wd[...])

    def second(p, hidden, dup, dgate):
        columns = slice(p * SUB_BACK, (p + 1) * SUB_BACK)
        here = pl.ds(pl.multiple_of(t * tile + p * SUB_BACK, SUB_BACK), SUB_BACK)
        dat_ref[:, here] += dot_t(wg[...], dgate) + dot_t(wu[...], dup)
        at = at_ref[:, columns]
        acc_g[...] += dot(at, dgate)
        acc_u[...] += dot(at, dup)
        acc_d[...] += dot(dyt_ref[:, columns], hidden)

    parts = tile // SUB_BACK
    ahead = first(0)
    for p in range(parts):
        now = ahead
        if p + 1 < parts:
            ahead = first(p + 1)
        second(p, *through(*now))

    def keep(tile_number):
        here = pl.ds(pl.multiple_of(tile_number * tile, tile), tile)
        return pltpu.make_async_copy(dat_kept, dat_out.at[:, here], dat_sem.at[tile_number])

    @pl.when((c == chunks - 1) & (t > 0))
    def _():
        keep(t - 1).wait()

    @pl.when(c == chunks - 1)
    def _():
        dat_kept[...] = dat_ref[:, pl.ds(pl.multiple_of(t * tile, tile), tile)].astype(BF16)
        keep(t).start()

    @pl.when((c == chunks - 1) & (t == tiles - 1))
    def _():
        keep(t).wait()

    def end(i):
        unpack(ring.finish(i, blocks.at[i]), n, *[out.at[i] for out in outs])

    @pl.when((c > 0) & (t == 0))
    def _():
        ring.pass_on(c - 1, blocks.at[c - 1])

    @pl.when((c == 2) & (t == 0))
    def _():
        for copy in spread():
            copy.wait_recv()
        for copy in spread_on():
            copy.start()

    @pl.when((c > 0) & (t == tiles - 1))
    def _():
        end(c - 1)

    @pl.when((c == 1) & (t == 0))
    def _():
        for copy in onward():
            copy.wait()

    @pl.when((c == 1) & (t == tiles - 1))
    def _():
        for k in range(2):
            for h in range(2):
                mine_ref[h, k] = outs[0][0, k, h * mine_ref.shape[2] : (h + 1) * mine_ref.shape[2], :]
        for copy in spread():
            copy.start()

    @pl.when((c == chunks - 1) & (t == tiles - 1))
    def _():
        for copy in spread():
            copy.wait_send()
        for copy in spread_on():
            copy.wait()

    @pl.when((c < chunks - 1) & (t == tiles - 1))
    def _():
        for s in range(3):
            pack(blocks.at[c], n, s, accs[s])
        ring.start(c, blocks.at[c])

    @pl.when((c == chunks - 1) & (t == tiles - 1))
    def _():
        for s in range(3):
            pack(last_ref, n, s, accs[s])


def outer_kernel(n, chunks, tiles, layer, *refs):
    refs = list(refs)
    take = lambda count: [refs.pop(0) for _ in range(count)]
    at_in, gate_ref, up_ref, dat_ref, h1t_ref, dyt_ref = take(6)
    w_refs = take(3)
    carried_ref = take(1)[0]
    outs = take(3)
    acc, acc_g, blocks, recv, summed, send_sem, recv_sem = take(7)
    wd_now, w_sem, at_ref, at_sem, dh_ref, dht_ref, dup_ref, carried_sem = take(8)

    c, t = pl.program_id(0), pl.program_id(1)
    tile = gate_ref.shape[0]
    ring = Ring(n, recv, summed, send_sem, recv_sem)
    whole = pltpu.make_async_copy(at_in, at_ref, at_sem)

    @pl.when((c == 0) & (t == 0))
    def _():
        carried = pltpu.make_async_copy(carried_ref, blocks.at[0], carried_sem)
        carried.start()
        whole.start()
        greet((ring.left, ring.right))
        greeted((ring.left, ring.right))
        carried.wait()
        ring.start(0, blocks.at[0])

    def weights(chunk, slot):
        return fetch(w_refs, layer, n, chunk, [None, None, wd_now.at[slot]], w_sem.at[slot])

    wd = wd_now.at[prefetch(weights, chunks, c, t)]

    @pl.when(t == 0)
    def _():
        acc[...] = jnp.zeros_like(acc)
        acc_g[...] = jnp.zeros_like(acc_g)

    @pl.when((c == 0) & (t < tiles))
    def _():
        width = 2 * LANES
        for p in range(tile // width):
            here = slice(p * width, (p + 1) * width)
            there = pl.ds(pl.multiple_of(t * tile + p * width, width), width)
            da = dat_ref[:, here].astype(F32)
            wide = h1t_ref[:, here].astype(F32)
            scale = lax.rsqrt(jnp.mean(wide * wide, 0, keepdims=True) + 1e-6)
            along = jnp.mean(da * wide, 0, keepdims=True)
            dwide = da * scale - wide * (scale * scale * scale * along)
            dht = (dyt_ref[:, here].astype(F32) + dwide.astype(BF16).astype(F32)).astype(BF16)
            dht_ref[:, there] = dht
            dh_ref[there, :] = dht.T

    @pl.when((c == 0) & (t == 0))
    def _():
        whole.wait()

    @pl.when(t < tiles)
    def _():
        def place(p):
            return pl.ds(pl.multiple_of(t * tile + p * SUB_BACK, SUB_BACK), SUB_BACK)

        def first(p):
            rows = slice(p * SUB_BACK, (p + 1) * SUB_BACK)
            return gate_ref[rows, :], up_ref[rows, :], dot_t(dh_ref[place(p), :], wd[...])

        parts = tile // SUB_BACK
        ahead = first(0)
        for p in range(parts):
            now = ahead
            if p + 1 < parts:
                ahead = first(p + 1)
            hidden, dup, dgate = through(*now)
            dup_ref[place(p), :] = dup
            acc[...] += dot(dht_ref[:, place(p)], hidden)
            acc_g[...] += dot(at_ref[:, place(p)], dgate)

    def end(i):
        unpack(ring.finish(i, blocks.at[i]), n, *[out.at[i] for out in outs])

    @pl.when((c == 0) & (t == 1))
    def _():
        ring.pass_on(0, blocks.at[0])

    @pl.when((c > 0) & (t == 0))
    def _():
        ring.pass_on(c, blocks.at[c], (2, 0))

    @pl.when((c > 0) & (t == 2))
    def _():
        ring.pass_on(c, blocks.at[c], (1,))

    i = c + 1
    here = blocks.at[i]

    @pl.when(t == tiles - 1)
    def _():
        pack(here, n, 2, acc)
        ring.start(i, here, (2,))
        pack(here, n, 0, acc_g)
        ring.start(i, here, (0,))

    @pl.when(t == tiles)
    def _():
        acc[...] = dot(at_ref[...], dup_ref[...])
        pack(here, n, 1, acc)
        ring.start(i, here, (1,))
        end(c)

    @pl.when((c == chunks - 1) & (t == tiles))
    def _():
        ring.pass_on(i, here, (2, 0, 1))
        end(i)


def sizes(n, w):
    d, ff = w[0].shape[1:]
    width, rows = n * LANES, 3 * (d // n // 2)
    return d, width, ff // width, (n, 2, rows, width)


def sums_of(count, d, n, width):
    shapes = ((count, 2, d // n, width), BF16), ((count, LANES, d), BF16), ((count, 8, LANES), F32)
    return [once(shape) for shape, _ in shapes], [jax.ShapeDtypeStruct(*one) for one in shapes]


def ring_scratch(count, packed):
    _, _, rows, width = packed
    return [
        pltpu.VMEM((count, 6, rows, width), BF16),
        pltpu.VMEM((count, 2, rows, width), BF16),
        pltpu.SemaphoreType.DMA((count, 3, 6)),
        pltpu.SemaphoreType.DMA((count, 3, 6)),
    ]


def once(shape):
    return pl.BlockSpec(shape, lambda c, t: (0,) * len(shape), pipeline_mode=pl.Buffered(1))


HBM = pl.BlockSpec(memory_space=pltpu.HBM)


def backward_inner(n, at, a, dy, dyt, w, near, layer, tile=2048, collective_id=0):
    tokens = at.shape[1]
    d, width, chunks, packed = sizes(n, w)
    tiles = tokens // tile
    straight = pl.BlockSpec((tile, d), lambda c, t: (t, 0))
    turned = pl.BlockSpec((d, tile), lambda c, t: (0, t))
    specs, shapes = sums_of(chunks - 1, d, n, width)
    early = (3, 2, 2, d // n // 2, width)
    *sums, last, dat, far, gradients = pl.pallas_call(
        functools.partial(inner_kernel, n, chunks, tiles, layer),
        grid=(chunks, tiles),
        in_specs=[turned, straight, straight, turned, HBM, HBM, HBM, HBM],
        out_specs=[*specs, once(packed), HBM, HBM, HBM],
        out_shape=[
            *shapes,
            jax.ShapeDtypeStruct(packed, BF16),
            jax.ShapeDtypeStruct((d, tokens), BF16),
            jax.ShapeDtypeStruct(near.shape[1:], F32),
            jax.ShapeDtypeStruct(early, BF16),
        ],
        scratch_shapes=[
            *[pltpu.VMEM((d, width), F32)] * 3,
            pltpu.VMEM((chunks - 1, *packed), BF16),
            *ring_scratch(chunks - 1, packed),
            pltpu.VMEM((2, width, d), BF16),
            pltpu.SemaphoreType.DMA((2, 3, n)),
            pltpu.VMEM((2, d, width), BF16),
            pltpu.VMEM((2, d, width), BF16),
            pltpu.VMEM((d, tokens), F32),
            pltpu.VMEM((d, tile), BF16),
            pltpu.SemaphoreType.DMA((tiles,)),
            pltpu.VMEM(early[1:], BF16),
            pltpu.SemaphoreType.DMA((6,)),
            pltpu.SemaphoreType.DMA((6,)),
        ],
        compiler_params=pltpu.CompilerParams(
            vmem_limit_bytes=VMEM_LIMIT, collective_id=collective_id, has_side_effects=True,
            dimension_semantics=("arbitrary", "arbitrary"),
        ),
        name="backward_inner",
    )(at, a, dy, dyt, *w, near)
    return sums, last, dat, far, gradients


def backward_outer(n, at, gate, up, dat, h1t, dyt, w, layer, carried, tile=1024, collective_id=1):
    tokens = at.shape[1]
    d, width, chunks, packed = sizes(n, w)
    tiles = tokens // tile
    at_first = pl.BlockSpec((d, tile), lambda c, t: (0, jnp.where(c == 0, jnp.minimum(t, tiles - 1), tiles - 1)))
    inside = pl.BlockSpec((None, tile, width), lambda c, t: (c, jnp.minimum(t, tiles - 1), 0))
    specs, shapes = sums_of(chunks + 1, d, n, width)
    return pl.pallas_call(
        functools.partial(outer_kernel, n, chunks, tiles, layer),
        grid=(chunks, tiles + 1),
        in_specs=[HBM, inside, inside, at_first, at_first, at_first, HBM, HBM, HBM, HBM],
        out_specs=specs,
        out_shape=shapes,
        scratch_shapes=[
            pltpu.VMEM((d, width), F32),
            pltpu.VMEM((d, width), F32),
            pltpu.VMEM((chunks + 1, *packed), BF16),
            *ring_scratch(chunks + 1, packed),
            pltpu.VMEM((2, width, d), BF16),
            pltpu.SemaphoreType.DMA((2, 3, n)),
            pltpu.VMEM((d, tokens), BF16),
            pltpu.SemaphoreType.DMA,
            pltpu.VMEM((tokens, d), BF16),
            pltpu.VMEM((d, tokens), BF16),
            pltpu.VMEM((tokens, width), BF16),
            pltpu.SemaphoreType.DMA,
        ],
        compiler_params=pltpu.CompilerParams(
            vmem_limit_bytes=VMEM_LIMIT, collective_id=collective_id, has_side_effects=True,
            dimension_semantics=("arbitrary", "arbitrary"),
        ),
        name="backward_outer",
    )(at, gate, up, dat, h1t, dyt, *w, carried)


def update_kernel(n, chunks, layers, count, *refs):
    refs = list(refs)
    take = lambda k: [refs.pop(0) for _ in range(k)]
    many = layers * chunks
    sums_in = [take(3), take(3)]
    near_in, far_in, early_in = take(3)
    w_in, m_in, v_in = take(3), take(3), take(3)
    w_out, m_own, v_own = take(3), take(3), take(3)
    gu_all, gd_all, squares = take(3)
    w_own = take(3)
    ss_mine, ss_all, ss_send, ss_recv = take(4)
    load_sem, sums_sem, gather_send, gather_recv = take(4)
    near, far, early, w_early, early_sem, w_sem = take(6)

    me = lax.axis_index(AXIS)
    right, left = (me + 1) % n, (me + n - 1) % n
    own_rows = [m.shape[1] for m in m_own]

    def mine(k, owner, h=None):
        rows = own_rows[k]
        if h is None:
            return pl.ds(pl.multiple_of(owner * rows, 16), rows)
        return pl.ds(pl.multiple_of(owner * rows + h * (rows // 2), 16), rows // 2)

    loads = []
    for k in range(3):
        for l in range(layers):
            i = len(loads)
            loads.append(
                (
                    pltpu.make_async_copy(w_in[k].at[l, mine(k, me)], w_own[k].at[l], load_sem.at[0, k, l]),
                    pltpu.make_async_copy(m_in[k].at[l], m_own[k].at[l], load_sem.at[1, k, l]),
                    pltpu.make_async_copy(v_in[k].at[l], v_own[k].at[l], load_sem.at[2, k, l]),
                )
            )
    sum_loads, done = [], 0
    for i, one in enumerate(sums_in):
        count_here = one[0].shape[0]
        for j, (src, dst) in enumerate(zip(one, (gu_all, gd_all, squares))):
            sum_loads.append(pltpu.make_async_copy(src, dst.at[pl.ds(done, count_here)], sums_sem.at[i, j]))
        done += count_here
    for copy in sum_loads:
        copy.start()
    at_once = layers - 1
    for copy in loads[at_once]:
        copy.start()
    own = w_in[0].shape[2] // n
    other_loads = [
        pltpu.make_async_copy(src, dst, early_sem.at[i])
        for i, (src, dst) in enumerate(((near_in, near), (far_in, far), (early_in, early)))
    ]
    for k in range(2):
        for o in range(n):
            there = pl.ds(o * own, LANES)
            other_loads.append(
                pltpu.make_async_copy(w_in[k].at[layers - 1, :, there], w_early.at[k, :, pl.ds(o * LANES, LANES)], w_sem.at[k, o])
            )
    peers = [(me + i) % n for i in range(1, n)]
    greet(peers)
    greeted(peers)
    for copy in sum_loads:
        copy.wait()

    total = squares[0]
    for i in range(1, many):
        total = total + squares[i]
    ss_mine[...] = total
    shares = [
        pltpu.make_async_remote_copy(
            src_ref=ss_mine, dst_ref=ss_all.at[i], send_sem=ss_send.at[i], recv_sem=ss_recv.at[i],
            device_id={AXIS: peer}, device_id_type=MESH,
        )
        for i, peer in enumerate(peers)
    ]
    for share in shares:
        share.start()
    for i, load in enumerate(loads):
        if i != at_once:
            for copy in load:
                copy.start()
    for copy in other_loads:
        copy.start()
    for share in shares:
        share.wait()
    for i in range(n - 1):
        total = total + ss_all[i]
    mean = jnp.sum(jnp.sum(total, axis=0, keepdims=True), axis=1, keepdims=True) / count
    factor = jnp.minimum(1.0, 0.5 * lax.rsqrt(mean + 1e-30))

    def gather(k, l, owner, h, way, to):
        rows = mine(k, owner, h)
        if l == layers - 1 and k < 2:
            places = [(rows, pl.ds(o * own + LANES, own - LANES)) for o in range(n)]
        else:
            places = [(rows, slice(None))]
        return [
            pltpu.make_async_remote_copy(
                src_ref=w_out[k].at[l, *place],
                dst_ref=w_out[k].at[l, *place],
                send_sem=gather_send.at[k, l, h, way, i],
                recv_sem=gather_recv.at[k, l, h, way, i],
                device_id={AXIS: to},
                device_id_type=MESH,
            )
            for i, place in enumerate(places)
        ]

    def own_send(k, l, h, way):
        return gather(k, l, me, h, way, (right, left)[way])

    def onward(k, l, way):
        owner, to = ((left, right), (right, left))[way]
        return gather(k, l, owner, way, 2, to)

    def adamw(w, m, v, g):
        w, g = w.astype(F32), g.astype(F32) * factor
        m = 0.9 * m + 0.1 * g
        v = 0.95 * v + 0.05 * g * g
        return (w - 0.02 * (m * lax.rsqrt(v + 1e-8) + 0.1 * w)).astype(BF16), m, v

    order = [(k, l) for l in reversed(range(layers)) for k in range(3)]
    for k, l in order:
        for copy in loads[k * layers + l]:
            copy.wait()
        base = (layers - 1 - l) * chunks

        def step(rows, columns, g):
            there = pl.ds(pl.multiple_of(me * own_rows[k] + rows.start, 16), rows.stop - rows.start)
            w_out[k][l, there, columns], m, v = adamw(w_own[k][l, rows, columns], m_own[k][l, rows, columns], v_own[k][l, rows, columns], g)
            m_own[k][l, rows, columns] = m
            v_own[k][l, rows, columns] = v

        for c in range(chunks):
            if k == 2:
                step(slice(c * LANES, (c + 1) * LANES), slice(None), gd_all[base + c])
            else:
                for o in range(n):
                    at = o * chunks * LANES + c * LANES
                    step(slice(0, own_rows[k]), slice(at, at + LANES), gu_all[base + c, k, :, o * LANES : (o + 1) * LANES])
        for h in range(2):
            for way in range(2):
                for copy in own_send(k, l, (h + way) % 2, way):
                    copy.start()
    for copy in other_loads:
        copy.wait()
    half = own_rows[0] // 2
    for r, owner in enumerate((left, right, (me + 2) % n)):
        for k in range(2):
            for h in range(2):
                rows, there = slice(h * half, (h + 1) * half), mine(k, owner, h)
                for o in range(n):
                    columns = slice(o * LANES, (o + 1) * LANES)
                    m, v = (near[r, j, k, rows, columns] if r < 2 else far[j, k, rows, columns] for j in range(2))
                    new, _, _ = adamw(w_early[k, there, columns], m, v, early[r, h, k, :, columns])
                    w_out[k][layers - 1, there, o * own : o * own + LANES] = new
    for k, l in order:
        for way in range(2):
            for copy in own_send(k, l, way, way):
                copy.wait_recv()
            for copy in onward(k, l, way):
                copy.start()
    for k, l in order:
        for way in range(2):
            for copy in own_send(k, l, 1 - way, way):
                copy.wait_recv()
            for copy in onward(k, l, way):
                copy.wait_recv()
                copy.wait_send()
            for h in range(2):
                for copy in own_send(k, l, h, way):
                    copy.wait_send()


def update(n, sums, others, w, m, v, collective_id):
    layers = w[0].shape[0]
    chunks = w[0].shape[2] // n // LANES
    count = sum(t.size for t in w)
    width = n * LANES
    vmem = pl.BlockSpec(memory_space=pltpu.VMEM)
    own = [t.shape for t in m]
    many = layers * chunks
    return pl.pallas_call(
        functools.partial(update_kernel, n, chunks, layers, count),
        in_specs=[HBM] * (len(sums) + 12),
        out_specs=[vmem] * 9,
        out_shape=[pltpu.VMEM(t.shape, t.dtype) for t in (*w, *m, *v)],
        scratch_shapes=[
            pltpu.VMEM((many, 2, w[0].shape[1] // n, width), BF16),
            pltpu.VMEM((many, LANES, w[0].shape[1]), BF16),
            pltpu.VMEM((many, 8, LANES), F32),
            *[pltpu.VMEM(s, BF16) for s in own],
            pltpu.VMEM((8, LANES), F32),
            pltpu.VMEM((n - 1, 8, LANES), F32),
            pltpu.SemaphoreType.DMA((n - 1,)),
            pltpu.SemaphoreType.DMA((n - 1,)),
            pltpu.SemaphoreType.DMA((3, 3, layers)),
            pltpu.SemaphoreType.DMA((2, 3)),
            pltpu.SemaphoreType.DMA((3, layers, 2, 3, n)),
            pltpu.SemaphoreType.DMA((3, layers, 2, 3, n)),
            *[pltpu.VMEM(t.shape, t.dtype) for t in others],
            pltpu.VMEM((2, w[0].shape[1], width), BF16),
            pltpu.SemaphoreType.DMA((3,)),
            pltpu.SemaphoreType.DMA((2, n)),
        ],
        compiler_params=pltpu.CompilerParams(vmem_limit_bytes=VMEM - RESERVE - sum(t.size * t.dtype.itemsize for t in (*w, *m, *v)), collective_id=collective_id, has_side_effects=True),
        name="update",
    )(*sums, *others, *w, *m, *v)


def put_kernel(count, *refs):
    sources, targets, sem = refs[:count], refs[count : 2 * count], refs[2 * count]
    copies = [pltpu.make_async_copy(a, b, sem.at[i]) for i, (a, b) in enumerate(zip(sources, targets))]
    for copy in copies:
        copy.start()
    for copy in copies:
        copy.wait()


def put(arrays):
    return pl.pallas_call(
        functools.partial(put_kernel, len(arrays)),
        in_specs=[pl.BlockSpec(memory_space=pltpu.VMEM)] * len(arrays),
        out_specs=[pl.BlockSpec(memory_space=pltpu.HBM)] * len(arrays),
        out_shape=[jax.ShapeDtypeStruct(t.shape, t.dtype) for t in arrays],
        scratch_shapes=[pltpu.SemaphoreType.DMA((len(arrays),))],
        compiler_params=pltpu.CompilerParams(vmem_limit_bytes=16 * 1024 * 1024),
        name="put",
    )(*arrays)


def solution(mesh):
    n = mesh.shape[AXIS]

    def step(x, dy, *arrays):
        w, m, v = arrays[:3], arrays[3:6], arrays[6:9]
        x, dy = x.reshape(x.shape[-2:]), dy.reshape(dy.shape[-2:])
        a1t, a2, a2t, h1t, dyt, *kept, near = forward(n, x, dy, w, (*m[:2], *v[:2]), 0, 1)
        sums2, last2, dat, far, early = backward_inner(n, a2t, a2, dy, dyt, w, near, 1)
        sums1 = backward_outer(n, a1t, *kept, dat, h1t, dyt, w, 0, last2)
        return tuple(put(update(n, [*sums2, *sums1], (near, far, early), w, m, v, 2)))

    whole, rows = P(None, None, None), P(None, AXIS, None)
    own, own_rows = P("rep", None, None), P("rep", AXIS, None)
    one = P(("rep", AXIS), None, None)
    return jax.shard_map(
        step,
        mesh=mesh,
        in_specs=(one, one, *[whole] * 3, *[rows] * 6),
        out_specs=(*[own] * 3, *[own_rows] * 6),
        check_vma=False,
    )
```
